128 devices in a mesh: data: 128 (over z, y, x, core).
Axes of the slice: x: 4, y: 4, z: 4, core: 2. Of those that a mesh axis runs over, the one named last changes fastest.
Arguments:
- x_now: bfloat16 [1024, 784, 128], P('data')
- labels_now: int32 [1024], P('data')
- x_next: bfloat16 [1024, 784, 128], P('data')
- up_one: float32 [2, 128, 512], replicated
- down_one: float32 [2, 512, 128], replicated
- merge_proj: float32 [512, 512], replicated
- up_two: float32 [2, 512, 2048], replicated
- down_two: float32 [2, 2048, 512], replicated
- head_proj: float32 [512, 1000], replicated
- vel_up_one: float32 [2, 128, 512], replicated
- vel_down_one: float32 [2, 512, 128], replicated
- vel_merge_proj: float32 [512, 512], replicated
- vel_up_two: float32 [2, 512, 2048], replicated
- vel_down_two: float32 [2, 2048, 512], replicated
- vel_head_proj: float32 [512, 1000], replicated
Outputs:
- output 1: float32 [1024, 1000], P('data')
- output 2: float32 [2, 128, 512], replicated
- output 3: float32 [2, 512, 128], replicated
- output 4: float32 [512, 512], replicated
- output 5: float32 [2, 512, 2048], replicated
- output 6: float32 [2, 2048, 512], replicated
- output 7: float32 [512, 1000], replicated
- output 8: float32 [2, 128, 512], replicated
- output 9: float32 [2, 512, 128], replicated
- output 10: float32 [512, 512], replicated
- output 11: float32 [2, 512, 2048], replicated
- output 12: float32 [2, 2048, 512], replicated
- output 13: float32 [512, 1000], replicated
All inputs are finite; a program needn't handle non-finite values.
Results may differ from the reference program's by a relative error of at most 0.0146127.
Values are sent between devices in bfloat16 or wider.
A program may use at most 1 GiB of HBM per device.

```python
import jax
import jax.numpy as jnp
from jax import lax

DATA_DEVS = 128
IMAGES_DEV = 8
TOKENS = 784
WIDTH = 128
DEPTH_ONE = 2
DEPTH_TWO = 2
CLASSES = 1000
BATCH = DATA_DEVS * IMAGES_DEV
MERGED = TOKENS // 4
WIDTH_TWO = 4 * WIDTH
HIDDEN_ONE = 4 * WIDTH
HIDDEN_TWO = 4 * WIDTH_TWO
MOMENTUM = 0.9
TRUST = 0.1
LN_EPS = 1e-6
SHIFT_SCALE = 1.5


def draw_weight(key_w, shape_w, fan_in, scale):
    return jax.random.normal(key_w, shape_w, jnp.float32) * (scale * fan_in ** -0.5)


def draw_images(key_img, key_shift):
    img_shift = jax.random.normal(key_shift, (BATCH, 1, WIDTH), jnp.float32) * SHIFT_SCALE
    raw_vals = jax.random.normal(key_img, (BATCH, TOKENS, WIDTH), jnp.float32)
    return (raw_vals + img_shift).astype(jnp.bfloat16)


def setup_inputs(seed: int = 0) -> dict:
    key_list = jax.random.split(jax.random.key(seed), 17)
    draw_specs = [
        ('up_one', (DEPTH_ONE, WIDTH, HIDDEN_ONE), WIDTH),
        ('down_one', (DEPTH_ONE, HIDDEN_ONE, WIDTH), HIDDEN_ONE),
        ('merge_proj', (4 * WIDTH, WIDTH_TWO), 4 * WIDTH),
        ('up_two', (DEPTH_TWO, WIDTH_TWO, HIDDEN_TWO), WIDTH_TWO),
        ('down_two', (DEPTH_TWO, HIDDEN_TWO, WIDTH_TWO), HIDDEN_TWO),
        ('head_proj', (WIDTH_TWO, CLASSES), WIDTH_TWO),
    ]
    drawn = {}
    drawn['x_now'] = draw_images(key_list[0], key_list[15])
    drawn['labels_now'] = jax.random.randint(key_list[1], (BATCH,), 0, CLASSES, jnp.int32)
    drawn['x_next'] = draw_images(key_list[2], key_list[16])
    for slot_num, spec_w in enumerate(draw_specs):
        drawn[spec_w[0]] = draw_weight(key_list[3 + slot_num], spec_w[1], spec_w[2], 1.0)
    for slot_num, spec_w in enumerate(draw_specs):
        drawn['vel_' + spec_w[0]] = draw_weight(key_list[9 + slot_num], spec_w[1], spec_w[2], TRUST)
    return drawn


def layer_norm(values):
    row_mean = jnp.mean(values, axis=-1, keepdims=True)
    centered = values - row_mean
    variance = jnp.mean(centered * centered, axis=-1, keepdims=True)
    return centered * lax.rsqrt(variance + LN_EPS)


def stage_block(residual, layer_weights):
    w_up, w_down = layer_weights
    normed = layer_norm(residual.astype(jnp.float32)).astype(jnp.bfloat16)
    pre_act = jnp.dot(normed, w_up.astype(jnp.bfloat16), preferred_element_type=jnp.float32)
    activated = jax.nn.gelu(pre_act, approximate=True).astype(jnp.bfloat16)
    block_out = jnp.dot(activated, w_down.astype(jnp.bfloat16), preferred_element_type=jnp.float32)
    return (residual.astype(jnp.float32) + block_out).astype(jnp.bfloat16), None


def model_logits(params, images):
    up_one, down_one, merge_proj, up_two, down_two, head_proj = params
    img_count = images.shape[0]
    residual = images.reshape(img_count * TOKENS, WIDTH)
    residual = lax.scan(stage_block, residual, (up_one, down_one))[0]
    merged = residual.reshape(img_count * MERGED, 4 * WIDTH)
    residual = jnp.dot(merged, merge_proj.astype(jnp.bfloat16), preferred_element_type=jnp.float32).astype(jnp.bfloat16)
    residual = lax.scan(stage_block, residual, (up_two, down_two))[0]
    pooled = jnp.mean(residual.reshape(img_count, MERGED, WIDTH_TWO).astype(jnp.float32), axis=1)
    normed = layer_norm(pooled).astype(jnp.bfloat16)
    return jnp.dot(normed, head_proj.astype(jnp.bfloat16), preferred_element_type=jnp.float32)


def shard_loss(params, images, labels):
    logits = model_logits(params, images)
    log_norm = jax.nn.logsumexp(logits, axis=-1)
    picked = jnp.sum(logits * jax.nn.one_hot(labels, CLASSES, dtype=jnp.float32), axis=-1)
    return jnp.sum(log_norm - picked) / BATCH


def lars_step(weight, velocity, grad_sum):
    red_axes = (weight.ndim - 2, weight.ndim - 1)
    w_norm = jnp.sqrt(jnp.sum(weight * weight, axis=red_axes, keepdims=True))
    g_norm = jnp.sqrt(jnp.sum(grad_sum * grad_sum, axis=red_axes, keepdims=True))
    new_vel = MOMENTUM * velocity + TRUST * (w_norm / g_norm) * grad_sum
    return weight - new_vel, new_vel


def reference(x_now, labels_now, x_next, up_one, down_one, merge_proj, up_two, down_two, head_proj, vel_up_one, vel_down_one, vel_merge_proj, vel_up_two, vel_down_two, vel_head_proj):
    params = (up_one, down_one, merge_proj, up_two, down_two, head_proj)
    grad_fn = jax.grad(shard_loss)

    def add_shard(running, shard_pair):
        grads = grad_fn(params, shard_pair[0], shard_pair[1])
        summed = jax.tree.map(lambda run_sum, shard_grad: run_sum + shard_grad.astype(jnp.bfloat16).astype(jnp.float32), running, grads)
        return summed, None

    zero_sums = jax.tree.map(jnp.zeros_like, params)
    img_shards = x_now.reshape(DATA_DEVS, IMAGES_DEV, TOKENS, WIDTH)
    label_shards = labels_now.reshape(DATA_DEVS, IMAGES_DEV)
    grad_sums = lax.scan(add_shard, zero_sums, (img_shards, label_shards))[0]
    new_up_one, new_vel_up_one = lars_step(up_one, vel_up_one, grad_sums[0])
    new_down_one, new_vel_down_one = lars_step(down_one, vel_down_one, grad_sums[1])
    new_merge_proj, new_vel_merge_proj = lars_step(merge_proj, vel_merge_proj, grad_sums[2])
    new_up_two, new_vel_up_two = lars_step(up_two, vel_up_two, grad_sums[3])
    new_down_two, new_vel_down_two = lars_step(down_two, vel_down_two, grad_sums[4])
    new_head_proj, new_vel_head_proj = lars_step(head_proj, vel_head_proj, grad_sums[5])
    new_params = (new_up_one, new_down_one, new_merge_proj, new_up_two, new_down_two, new_head_proj)
    next_shards = x_next.reshape(DATA_DEVS, IMAGES_DEV, TOKENS, WIDTH)
    logits_next = lax.map(lambda images: model_logits(new_params, images), next_shards).reshape(BATCH, CLASSES)
    return (logits_next, new_up_one, new_down_one, new_merge_proj, new_up_two, new_down_two, new_head_proj, new_vel_up_one, new_vel_down_one, new_vel_merge_proj, new_vel_up_two, new_vel_down_two, new_vel_head_proj)
```

```python
import functools

import jax
import jax.numpy as jnp
from jax import lax
from jax.experimental import pallas as pl
from jax.experimental.pallas import tpu as pltpu
from jax.sharding import PartitionSpec as P

MOMENTUM = 0.9
TRUST = 0.1
LN_EPS = 1e-6
GELU_A = 0.7978845608028654
GELU_B = GELU_A * 0.044715
ROWS = 1568
ROWS_PAD = 1792
PER_IMAGE = 196
W1 = 128
W2 = 512
H1 = 512
H2 = 2048
CHUNK = 256
NCH = H2 // CHUNK
TILE = 224
NT = ROWS // TILE
SPLIT = 784
VMEM_LIMIT = 63 * 1024 * 1024
F32 = jnp.float32
BF16 = jnp.bfloat16


def dot_nn(lhs, rhs):
    return lax.dot_general(lhs, rhs, (((1,), (0,)), ((), ())), preferred_element_type=F32)


def dot_nt(lhs, rhs):
    return lax.dot_general(lhs, rhs, (((1,), (1,)), ((), ())), preferred_element_type=F32)


def dot_tn(lhs, rhs):
    return lax.dot_general(lhs, rhs, (((0,), (0,)), ((), ())), preferred_element_type=F32)


def ln_parts(values):
    row_mean = jnp.mean(values, axis=-1, keepdims=True)
    centered = values - row_mean
    variance = jnp.mean(centered * centered, axis=-1, keepdims=True)
    inv = lax.rsqrt(variance + LN_EPS)
    return centered * inv, inv


def ln_back(normed, inv, grad):
    mean_grad = jnp.mean(grad, axis=-1, keepdims=True)
    mean_dot = jnp.mean(grad * normed, axis=-1, keepdims=True)
    return inv * (grad - mean_grad - normed * mean_dot)


def gelu_fwd(pre):
    sq = pre * pre
    tan = jnp.tanh(pre * (GELU_A + GELU_B * sq))
    half = 0.5 * pre
    return half + half * tan


def gelu_both(pre):
    sq = pre * pre
    tan = jnp.tanh(pre * (GELU_A + GELU_B * sq))
    half = 0.5 * pre
    act = half + half * tan
    slope = (0.5 + 0.5 * tan) + (half * (1.0 - tan * tan)) * (GELU_A + (3.0 * GELU_B) * sq)
    return act, slope


def fold_sq(mat):
    rows, cols = mat.shape
    return jnp.sum((mat * mat).reshape(rows // 8, 8, cols), axis=0)


def lars_block(weight, vel, grad, scale):
    new_vel = MOMENTUM * vel + scale * grad.astype(F32)
    return weight - new_vel, new_vel


def params(**kwargs):
    return pltpu.CompilerParams(vmem_limit_bytes=VMEM_LIMIT, **kwargs)


def whole(shape):
    zeros = (0,) * len(shape)
    return pl.BlockSpec(shape, lambda *_: zeros)


def stage_one_tile(x_tile, ub, vb, mb):
    outs0, outs1 = [], []
    for quarter in range(4):
        resid = x_tile[:, quarter * W1:(quarter + 1) * W1]
        for layer in range(2):
            normed = ln_parts(resid.astype(F32))[0].astype(BF16)
            act = gelu_fwd(dot_nn(normed, ub[layer])).astype(BF16)
            resid = (resid.astype(F32) + dot_nn(act, vb[layer])).astype(BF16)
            (outs0, outs1)[layer].append(resid)
    mid = jnp.concatenate(outs0, axis=1)
    merged = jnp.concatenate(outs1, axis=1)
    return mid, merged, dot_nn(merged, mb[...]).astype(BF16)


def stage_one_now(x, up_one, down_one, merge):
    def kernel(x_ref, u_ref, v_ref, m_ref, mid_ref, merged_ref, res_ref, ub_ref, vb_ref, mb_ref, su_ref, sv_ref, sm_ref):
        @pl.when(pl.program_id(0) == 0)
        def _():
            ub_ref[...] = u_ref[...].astype(BF16)
            vb_ref[...] = v_ref[...].astype(BF16)
            mb_ref[...] = m_ref[...].astype(BF16)
            for layer in range(2):
                su_ref[layer] = fold_sq(u_ref[layer])
                sv_ref[layer] = fold_sq(v_ref[layer])
            sm_ref[...] = fold_sq(m_ref[...])

        mid, merged, res = stage_one_tile(x_ref[...], ub_ref, vb_ref, mb_ref)
        mid_ref[...] = mid
        merged_ref[...] = merged
        res_ref[...] = res

    tile = pl.BlockSpec((TILE, W2), lambda i: (i, 0))
    act = jax.ShapeDtypeStruct((ROWS, W2), BF16)
    small = [((2, W1, H1), BF16), ((2, H1, W1), BF16), ((W2, W2), BF16), ((2, 8, H1), F32), ((2, 8, W1), F32), ((8, W2), F32)]
    return pl.pallas_call(
        kernel,
        grid=(NT,),
        in_specs=[tile, whole((2, W1, H1)), whole((2, H1, W1)), whole((W2, W2))],
        out_specs=[tile] * 3 + [whole(s) for s, _ in small],
        out_shape=[act] * 3 + [jax.ShapeDtypeStruct(s, d) for s, d in small],
        compiler_params=params(),
        name="stage_one_now",
    )(x, up_one, down_one, merge)


def stage_one_next(x, scales, weights, vels, grads):
    def kernel(sc_ref, x_ref, u_ref, v_ref, m_ref, pu_ref, pv_ref, pm_ref, gu_ref, gv_ref, gm_ref, res_ref, nu_ref, nv_ref, nm_ref, qu_ref, qv_ref, qm_ref, ub_ref, vb_ref, mb_ref):
        @pl.when(pl.program_id(0) == 0)
        def _():
            for layer in range(2):
                nu_ref[layer], qu_ref[layer] = lars_block(u_ref[layer], pu_ref[layer], gu_ref[layer], sc_ref[layer])
                nv_ref[layer], qv_ref[layer] = lars_block(v_ref[layer], pv_ref[layer], gv_ref[layer], sc_ref[2 + layer])
            nm_ref[...], qm_ref[...] = lars_block(m_ref[...], pm_ref[...], gm_ref[...], sc_ref[4])
            ub_ref[...] = nu_ref[...].astype(BF16)
            vb_ref[...] = nv_ref[...].astype(BF16)
            mb_ref[...] = nm_ref[...].astype(BF16)

        res_ref[...] = stage_one_tile(x_ref[...], ub_ref, vb_ref, mb_ref)[2]

    tile = pl.BlockSpec((TILE, W2), lambda i: (i, 0))
    shapes = [(2, W1, H1), (2, H1, W1), (W2, W2)]
    return pl.pallas_call(
        kernel,
        grid=(NT,),
        in_specs=[pl.BlockSpec(memory_space=pltpu.SMEM), tile] + [whole(s) for s in shapes] * 3,
        out_specs=[tile] + [whole(s) for s in shapes] * 2,
        out_shape=[jax.ShapeDtypeStruct((ROWS, W2), BF16)] + [jax.ShapeDtypeStruct(s, F32) for s in shapes] * 2,
        scratch_shapes=[pltpu.VMEM(s, BF16) for s in shapes],
        compiler_params=params(),
        name="stage_one_next",
    )(scales, x, *weights, *vels, *grads)


def row_parts():
    return [(start, SPLIT) for start in range(0, ROWS, SPLIT)]


def stage_two_start(chunk, src_ref, dst_norm, acc_ref):
    for start, size in row_parts():
        resid = src_ref[start:start + size].astype(F32)
        dst_norm[start:start + size] = ln_parts(resid)[0].astype(BF16)
        acc_ref[start:start + size] = resid


def stage_two_step(norm_ref, acc_ref, ub, vb):
    for start, size in row_parts():
        act = gelu_fwd(dot_nn(norm_ref[start:start + size], ub)).astype(BF16)
        acc_ref[start:start + size] += dot_nn(act, vb)


def pool_images(resid_ref, pool_ref):
    cols = lax.broadcasted_iota(jnp.int32, (16, ROWS_PAD), 1)
    base = lax.broadcasted_iota(jnp.int32, (16, ROWS_PAD), 0) * PER_IMAGE
    mask = ((cols >= base) & (cols < base + PER_IMAGE) & (cols < ROWS)).astype(F32).astype(BF16)
    pool_ref[...] = dot_nn(mask, resid_ref[...]) * (1.0 / PER_IMAGE)


def stage_two_now(res_in, up_two, down_two):
    def kernel(r_ref, u_ref, v_ref, mid_ref, ub_ref, vb_ref, su_ref, sv_ref, pool_ref, norm_s, acc_s, res_s):
        layer, chunk = pl.program_id(0), pl.program_id(1)

        @pl.when(chunk == 0)
        def _():
            @pl.when(layer == 0)
            def _():
                stage_two_start(chunk, r_ref, norm_s, acc_s)

            @pl.when(layer == 1)
            def _():
                stage_two_start(chunk, mid_ref, norm_s, acc_s)
            su_ref[...] = jnp.zeros_like(su_ref)
            sv_ref[...] = jnp.zeros_like(sv_ref)

        ub = u_ref[0].astype(BF16)
        vb = v_ref[0].astype(BF16)
        ub_ref[0] = ub
        vb_ref[0] = vb
        su_ref[0] += fold_sq(u_ref[0])
        sv_ref[0] += fold_sq(v_ref[0])
        stage_two_step(norm_s, acc_s, ub, vb)

        @pl.when((chunk == NCH - 1) & (layer == 0))
        def _():
            mid_ref[...] = acc_s[...].astype(BF16)

        @pl.when((chunk == NCH - 1) & (layer == 1))
        def _():
            res_s[:ROWS] = acc_s[...].astype(BF16)
            res_s[ROWS:] = jnp.zeros((ROWS_PAD - ROWS, W2), BF16)
            pool_images(res_s, pool_ref)

    u_spec = pl.BlockSpec((1, W2, CHUNK), lambda l, j: (l, 0, j))
    v_spec = pl.BlockSpec((1, CHUNK, W2), lambda l, j: (l, j, 0))
    return pl.pallas_call(
        kernel,
        grid=(2, NCH),
        in_specs=[whole((ROWS, W2)), u_spec, v_spec],
        out_specs=[whole((ROWS, W2)), u_spec, v_spec, pl.BlockSpec((1, 8, CHUNK), lambda l, j: (l, 0, 0)), pl.BlockSpec((1, 8, W2), lambda l, j: (l, 0, 0)), whole((16, W2))],
        out_shape=[jax.ShapeDtypeStruct((ROWS, W2), BF16), jax.ShapeDtypeStruct((2, W2, H2), BF16), jax.ShapeDtypeStruct((2, H2, W2), BF16), jax.ShapeDtypeStruct((2, 8, CHUNK), F32), jax.ShapeDtypeStruct((2, 8, W2), F32), jax.ShapeDtypeStruct((16, W2), F32)],
        scratch_shapes=[pltpu.VMEM((ROWS, W2), BF16), pltpu.VMEM((ROWS, W2), F32), pltpu.VMEM((ROWS_PAD, W2), BF16)],
        compiler_params=params(),
        name="stage_two_now",
    )(res_in, up_two, down_two)


def stage_two_next(res_in, scales, up_two, down_two, vel_up, vel_down, grad_up, grad_down):
    def kernel(sc_ref, r_ref, u_ref, v_ref, pu_ref, pv_ref, gu_ref, gv_ref, nu_ref, nv_ref, qu_ref, qv_ref, pool_ref, norm_s, acc_s, res_s):
        layer, chunk = pl.program_id(0), pl.program_id(1)

        @pl.when(chunk == 0)
        def _():
            @pl.when(layer == 0)
            def _():
                stage_two_start(chunk, r_ref, norm_s, acc_s)

            @pl.when(layer == 1)
            def _():
                stage_two_start(chunk, res_s, norm_s, acc_s)

        new_u, new_pu = lars_block(u_ref[0], pu_ref[0], gu_ref[0], sc_ref[layer])
        new_v, new_pv = lars_block(v_ref[0], pv_ref[0], gv_ref[0], sc_ref[2 + layer])
        nu_ref[0] = new_u
        qu_ref[0] = new_pu
        nv_ref[0] = new_v
        qv_ref[0] = new_pv
        stage_two_step(norm_s, acc_s, new_u.astype(BF16), new_v.astype(BF16))

        @pl.when(chunk == NCH - 1)
        def _():
            res_s[:ROWS] = acc_s[...].astype(BF16)

            @pl.when(layer == 1)
            def _():
                res_s[ROWS:] = jnp.zeros((ROWS_PAD - ROWS, W2), BF16)
                pool_images(res_s, pool_ref)

    u_spec = pl.BlockSpec((1, W2, CHUNK), lambda l, j: (l, 0, j))
    v_spec = pl.BlockSpec((1, CHUNK, W2), lambda l, j: (l, j, 0))
    return pl.pallas_call(
        kernel,
        grid=(2, NCH),
        in_specs=[pl.BlockSpec(memory_space=pltpu.SMEM), whole((ROWS, W2))] + [u_spec, v_spec] * 3,
        out_specs=[u_spec, v_spec] * 2 + [whole((16, W2))],
        out_shape=[jax.ShapeDtypeStruct((2, W2, H2), F32), jax.ShapeDtypeStruct((2, H2, W2), F32)] * 2 + [jax.ShapeDtypeStruct((16, W2), F32)],
        scratch_shapes=[pltpu.VMEM((ROWS, W2), BF16), pltpu.VMEM((ROWS, W2), F32), pltpu.VMEM((ROWS_PAD, W2), BF16)],
        compiler_params=params(),
        name="stage_two_next",
    )(scales, res_in, up_two, down_two, vel_up, vel_down, grad_up, grad_down)


def stage_two_back(grad_pool, res_in, res_mid, merged, up_b, down_b, merge_b):
    def kernel(gp_ref, r0_ref, r1_ref, m_ref, u_ref, v_ref, mw_ref, du_ref, dv_ref, dm_ref, gout_ref, g_s, gt_s, n_s, nt_s, act_s, pre_s, dn_s):
        step, chunk = pl.program_id(0), pl.program_id(1)

        @pl.when((step == 0) & (chunk == 0))
        def _():
            rows = lax.broadcasted_iota(jnp.int32, (ROWS, 128), 0)
            base = lax.broadcasted_iota(jnp.int32, (ROWS, 128), 1) * PER_IMAGE
            mask = ((rows >= base) & (rows < base + PER_IMAGE)).astype(F32).astype(BF16)
            g_s[...] = dot_nn(mask, gp_ref[...]).astype(BF16)
            zeros = jnp.zeros((W2, ROWS_PAD - 1536), BF16)
            gt_s[:, 1536:] = zeros
            nt_s[:, 1536:] = zeros
            gt_s[:, :ROWS] = g_s[...].T
            act_s[ROWS:] = jnp.zeros((ROWS_PAD - ROWS, CHUNK), BF16)
            pre_s[ROWS:] = jnp.zeros((ROWS_PAD - ROWS, CHUNK), BF16)

        def begin(src_ref):
            n_s[...] = ln_parts(src_ref[...].astype(F32))[0].astype(BF16)
            nt_s[:, :ROWS] = n_s[...].T
            dn_s[...] = jnp.zeros_like(dn_s)

        @pl.when((step == 0) & (chunk == 0))
        def _():
            begin(r1_ref)

        @pl.when((step == 1) & (chunk == 0))
        def _():
            begin(r0_ref)

        ub = u_ref[0]
        vb = v_ref[0]
        for start, size in row_parts():
            act, slope = gelu_both(dot_nn(n_s[start:start + size], ub))
            grad_pre = (dot_nt(g_s[start:start + size], vb) * slope).astype(BF16)
            act_s[start:start + size] = act.astype(BF16)
            pre_s[start:start + size] = grad_pre
            dn_s[start:start + size] += dot_nt(grad_pre, ub)
        du_ref[0] = dot_nn(nt_s[...], pre_s[...]).astype(BF16)
        dv_ref[0] = dot_nn(gt_s[...], act_s[...]).T.astype(BF16)

        def finish(src_ref):
            normed, inv = ln_parts(src_ref[...].astype(F32))
            g_s[...] = (ln_back(normed, inv, dn_s[...]) + g_s[...].astype(F32)).astype(BF16)

        @pl.when((step == 0) & (chunk == NCH - 1))
        def _():
            finish(r1_ref)
            gt_s[:, :ROWS] = g_s[...].T

        @pl.when((step == 1) & (chunk == NCH - 1))
        def _():
            finish(r0_ref)
            gout_ref[...] = dot_nt(g_s[...], mw_ref[...]).astype(BF16)
            dm_ref[...] = dot_tn(m_ref[...], g_s[...]).astype(BF16)

    u_spec = pl.BlockSpec((1, W2, CHUNK), lambda l, j: (1 - l, 0, j))
    v_spec = pl.BlockSpec((1, CHUNK, W2), lambda l, j: (1 - l, j, 0))
    act = whole((ROWS, W2))
    return pl.pallas_call(
        kernel,
        grid=(2, NCH),
        in_specs=[whole((128, W2)), act, act, act, u_spec, v_spec, whole((W2, W2))],
        out_specs=[u_spec, v_spec, whole((W2, W2)), act],
        out_shape=[jax.ShapeDtypeStruct((2, W2, H2), BF16), jax.ShapeDtypeStruct((2, H2, W2), BF16), jax.ShapeDtypeStruct((W2, W2), BF16), jax.ShapeDtypeStruct((ROWS, W2), BF16)],
        scratch_shapes=[pltpu.VMEM((ROWS, W2), BF16), pltpu.VMEM((W2, ROWS_PAD), BF16), pltpu.VMEM((ROWS, W2), BF16), pltpu.VMEM((W2, ROWS_PAD), BF16), pltpu.VMEM((ROWS_PAD, CHUNK), BF16), pltpu.VMEM((ROWS_PAD, CHUNK), BF16), pltpu.VMEM((ROWS, W2), F32)],
        compiler_params=params(),
        name="stage_two_back",
    )(grad_pool, res_in, res_mid, merged, up_b, down_b, merge_b)


def stage_one_back(grad_in, x, mid, up_b, down_b):
    def kernel(g_ref, x_ref, mid_ref, u_ref, v_ref, du_ref, dv_ref, du_s, dv_s):
        tile_id = pl.program_id(0)

        @pl.when(tile_id == 0)
        def _():
            du_s[...] = jnp.zeros_like(du_s)
            dv_s[...] = jnp.zeros_like(dv_s)

        for quarter in range(4):
            cols = slice(quarter * W1, (quarter + 1) * W1)
            grad = g_ref[:, cols]
            for layer in (1, 0):
                resid = (mid_ref if layer else x_ref)[:, cols]
                normed, inv = ln_parts(resid.astype(F32))
                normed_b = normed.astype(BF16)
                act, slope = gelu_both(dot_nn(normed_b, u_ref[layer]))
                grad_pre = (dot_nt(grad, v_ref[layer]) * slope).astype(BF16)
                du_s[layer] += dot_tn(normed_b, grad_pre)
                dv_s[layer] += dot_tn(grad, act.astype(BF16))
                if layer:
                    grad_norm = dot_nt(grad_pre, u_ref[layer])
                    grad = (ln_back(normed, inv, grad_norm) + grad.astype(F32)).astype(BF16)

        @pl.when(tile_id == NT - 1)
        def _():
            du_ref[...] = du_s[...].astype(BF16)
            for layer in range(2):
                dv_ref[layer] = dv_s[layer].T.astype(BF16)

    tile = pl.BlockSpec((TILE, W2), lambda i: (i, 0))
    return pl.pallas_call(
        kernel,
        grid=(NT,),
        in_specs=[tile, tile, tile, whole((2, W1, H1)), whole((2, H1, W1))],
        out_specs=[whole((2, W1, H1)), whole((2, H1, W1))],
        out_shape=[jax.ShapeDtypeStruct((2, W1, H1), BF16), jax.ShapeDtypeStruct((2, H1, W1), BF16)],
        scratch_shapes=[pltpu.VMEM((2, W1, H1), F32), pltpu.VMEM((2, W1, H1), F32)],
        compiler_params=params(),
        name="stage_one_back",
    )(grad_in, x, mid, up_b, down_b)


def head_and_loss(pooled, labels, head_b, global_batch):
    normed, inv = ln_parts(pooled)
    head_in = normed.astype(BF16)
    logits = jnp.dot(head_in, head_b, preferred_element_type=F32)
    probs = jax.nn.softmax(logits, axis=-1)
    class_ids = jnp.arange(logits.shape[1], dtype=jnp.int32)
    onehot = (labels[:, None] == class_ids[None, :]).astype(F32)
    grad_logits = ((probs - onehot) / global_batch).astype(BF16)
    grad_head = dot_tn(head_in, grad_logits).astype(BF16)
    grad_pool = ln_back(normed, inv, dot_nt(grad_logits, head_b)) / PER_IMAGE
    return grad_head, grad_pool.astype(BF16)


def total_sq(grad):
    grad_f = grad.astype(F32)
    return jnp.sum(grad_f * grad_f, axis=(-2, -1))


def solution(mesh):
    data_devs = mesh.shape['data']

    def local_step(x_now, labels_now, x_next, up_one, down_one, merge_proj, up_two, down_two, head_proj, vel_up_one, vel_down_one, vel_merge_proj, vel_up_two, vel_down_two, vel_head_proj):
        images = x_now.shape[0]
        xn = x_now.reshape(ROWS, W2)
        xf = x_next.reshape(ROWS, W2)
        mid, merged, res0, ub1, vb1, mb, su1, sv1, sm = stage_one_now(xn, up_one, down_one, merge_proj)
        res1, ub2, vb2, su2, sv2, pooled = stage_two_now(res0, up_two, down_two)
        grad_head, grad_pool = head_and_loss(pooled[:images], labels_now, head_proj.astype(BF16), images * data_devs)
        grad_pool = jnp.pad(grad_pool, ((0, 128 - images), (0, 0)))
        du2, dv2, dm, grad_mid = stage_two_back(grad_pool, res0, res1, merged, ub2, vb2, mb)
        du1, dv1 = stage_one_back(grad_mid, xn, mid, ub1, vb1)
        du1, dv1, dm, du2, dv2, dh = lax.psum((du1, dv1, dm, du2, dv2, grad_head), 'data')
        sq = lambda folded: jnp.sum(folded, axis=(-2, -1))
        scale = lambda w_sq, g_sq: TRUST * (jnp.sqrt(w_sq) / jnp.sqrt(g_sq))
        scales_one = jnp.concatenate([scale(sq(su1), total_sq(du1)), scale(sq(sv1), total_sq(dv1)), scale(sq(sm), total_sq(dm))[None]])
        scales_two = jnp.concatenate([scale(sq(su2), total_sq(du2)), scale(sq(sv2), total_sq(dv2))])
        res_f, nu1, nv1, nm, qu1, qv1, qm = stage_one_next(xf, scales_one, (up_one, down_one, merge_proj), (vel_up_one, vel_down_one, vel_merge_proj), (du1, dv1, dm))
        nu2, nv2, qu2, qv2, pooled_f = stage_two_next(res_f, scales_two, up_two, down_two, vel_up_two, vel_down_two, du2, dv2)
        nh, qh = lars_block(head_proj, vel_head_proj, dh, scale(jnp.sum(head_proj * head_proj), total_sq(dh)))
        logits = jnp.dot(ln_parts(pooled_f[:images])[0].astype(BF16), nh.astype(BF16), preferred_element_type=F32)
        return logits, nu1, nv1, nm, nu2, nv2, nh, qu1, qv1, qm, qu2, qv2, qh

    batch_split = P('data')
    in_specs = (batch_split,) * 3 + (P(),) * 12
    out_specs = (batch_split,) + (P(),) * 12
    return jax.shard_map(local_step, mesh=mesh, in_specs=in_specs, out_specs=out_specs, check_vma=False)
```

```python
import functools

import jax
import jax.numpy as jnp
from jax import lax
from jax.experimental import pallas as pl
from jax.experimental.pallas import tpu as pltpu
from jax.sharding import PartitionSpec as P

MOMENTUM = 0.9
TRUST = 0.1
LN_EPS = 1e-6
GELU_A = 2.0 * 0.7978845608028654
GELU_B = 4.0 * GELU_A * 0.044715
UNIT = 16
LANES = 128
UNIT_SIZE = UNIT * LANES
ROWS = 1568
ROWS_PAD = 1792
PER_IMAGE = 196
W1 = 128
W2 = 512
H1 = 512
H2 = 2048
CHUNK = 512
NCH = H2 // CHUNK
FCHUNK = 1024
NF = H2 // FCHUNK
TILE = 784
NT = ROWS // TILE
TOKENS = 4 * TILE
SPLITS = (784, 784)
HEAD_PAD = 1024
HEAD_ROWS = HEAD_PAD // (2 * NF)
HEAD_UNITS = HEAD_ROWS * W2 // UNIT_SIZE
HERE_AXES = (0, 1)
CHUNK_UNITS = CHUNK * W2 // UNIT_SIZE
F_UNITS = FCHUNK * W2 // UNIT_SIZE
SCALE_SHAPE = (UNIT, LANES)
ONE_SHAPES = [(2, W1, H1), (2, H1, W1), (W2, W2)]
UP_SHAPE, DOWN_SHAPE = (2, W2, H2), (2, H2, W2)
VMEM_LIMIT = 63 * 1024 * 1024
F32 = jnp.float32
BF16 = jnp.bfloat16


def dot_nn(lhs, rhs):
    return lax.dot_general(lhs, rhs, (((1,), (0,)), ((), ())), preferred_element_type=F32)


def dot_nt(lhs, rhs):
    return lax.dot_general(lhs, rhs, (((1,), (1,)), ((), ())), preferred_element_type=F32)


def dot_tn(lhs, rhs):
    return lax.dot_general(lhs, rhs, (((0,), (0,)), ((), ())), preferred_element_type=F32)


def ln_parts(values):
    row_mean = jnp.mean(values, axis=-1, keepdims=True)
    centered = values - row_mean
    variance = jnp.mean(centered * centered, axis=-1, keepdims=True)
    inv = lax.rsqrt(variance + LN_EPS)
    return centered * inv, inv


def ln_back(normed, inv, grad):
    mean_grad = jnp.mean(grad, axis=-1, keepdims=True)
    mean_dot = jnp.mean(grad * normed, axis=-1, keepdims=True)
    return inv * (grad - mean_grad - normed * mean_dot)


def gelu_fwd(half):
    tan = jnp.tanh(half * (GELU_A + GELU_B * (half * half)))
    return half + half * tan


def gelu_both(half):
    sq = half * half
    tan = jnp.tanh(half * (GELU_A + GELU_B * sq))
    above = 1.0 + tan
    return half * above, above * (1.0 + (half * (1.0 - tan)) * (GELU_A + (3.0 * GELU_B) * sq))


def halve(weight):
    return (0.5 * weight).astype(BF16)


def fold_sq(mat):
    rows, cols = mat.shape
    return jnp.sum((mat * mat).reshape(rows // 8, 8, cols), axis=0)


def lars_block(weight, vel, grad, scale):
    new_vel = MOMENTUM * vel + scale * grad.astype(F32)
    return weight - new_vel, new_vel


def put_units(ref, start, mat):
    rows, cols = mat.shape
    groups = rows // UNIT
    for lane in range(cols // LANES):
        ref[pl.ds(start + lane * groups, groups)] = mat[:, lane * LANES:(lane + 1) * LANES].reshape(groups, UNIT, LANES)


def get_units(ref, start, rows, cols):
    groups = rows // UNIT
    parts = [ref[pl.ds(start + lane * groups, groups)].reshape(rows, LANES) for lane in range(cols // LANES)]
    return parts[0] if len(parts) == 1 else jnp.concatenate(parts, axis=1)


struct = jax.ShapeDtypeStruct


def unit_struct(count):
    return struct((count, UNIT, LANES), BF16)


def params(**kwargs):
    return pltpu.CompilerParams(vmem_limit_bytes=VMEM_LIMIT, **kwargs)


def whole(shape):
    zeros = (0,) * len(shape)
    return pl.BlockSpec(shape, lambda *_: zeros)


def token_parts(x_ref, x_s):
    x_s[...] = x_ref[...].astype(F32)
    return [x_s[pl.ds(quarter, TILE, stride=4), :] for quarter in range(4)]


def stage_one_tile(parts, ub, vb, mb):
    outs0, outs1 = [], []
    for resid in parts:
        for layer in range(2):
            normed = ln_parts(resid.astype(F32))[0].astype(BF16)
            act = gelu_fwd(dot_nn(normed, ub[layer])).astype(BF16)
            resid = (resid.astype(F32) + dot_nn(act, vb[layer])).astype(BF16)
            (outs0, outs1)[layer].append(resid)
    mid = jnp.concatenate(outs0, axis=1)
    merged = jnp.concatenate(outs1, axis=1)
    return mid, merged, dot_nn(merged, mb[...]).astype(BF16)


def rows_spec(rows, cols):
    return pl.BlockSpec((rows, cols), lambda i: (i, 0))


def stage_one_now(x, up_one, down_one, merge):
    def kernel(x_ref, u_ref, v_ref, m_ref, mid_ref, merged_ref, res_ref, ub_ref, vb_ref, mb_ref, su_ref, sv_ref, sm_ref, x_s):
        @pl.when(pl.program_id(0) == 0)
        def _():
            ub_ref[...] = halve(u_ref[...])
            vb_ref[...] = v_ref[...].astype(BF16)
            mb_ref[...] = m_ref[...].astype(BF16)
            for layer in range(2):
                su_ref[layer] = fold_sq(u_ref[layer])
                sv_ref[layer] = fold_sq(v_ref[layer])
            sm_ref[...] = fold_sq(m_ref[...])

        mid, merged, res = stage_one_tile(token_parts(x_ref, x_s), ub_ref, vb_ref, mb_ref)
        mid_ref[...] = mid
        merged_ref[...] = merged
        res_ref[...] = res

    tile = rows_spec(TILE, W2)
    act = struct((ROWS, W2), BF16)
    small = [(shape, BF16) for shape in ONE_SHAPES] + [((2, 8, H1), F32), ((2, 8, W1), F32), ((8, W2), F32)]
    return pl.pallas_call(
        kernel,
        grid=(NT,),
        in_specs=[rows_spec(TOKENS, W1)] + [whole(s) for s in ONE_SHAPES],
        out_specs=[tile] * 3 + [whole(s) for s, _ in small],
        out_shape=[act] * 3 + [struct(s, d) for s, d in small],
        scratch_shapes=[pltpu.VMEM((TOKENS, W1), F32)],
        compiler_params=params(),
        name="stage_one_now",
    )(x, up_one, down_one, merge)


def stage_one_next(x, scales, grads, weights, vels):
    def kernel(sc_ref, x_ref, u_ref, v_ref, m_ref, pu_ref, pv_ref, pm_ref, gu_ref, gv_ref, gm_ref, res_ref, nu_ref, nv_ref, nm_ref, qu_ref, qv_ref, qm_ref, ub_ref, vb_ref, mb_ref, x_s):
        @pl.when(pl.program_id(0) == 0)
        def _():
            for layer in range(2):
                nu_ref[layer], qu_ref[layer] = lars_block(u_ref[layer], pu_ref[layer], get_units(gu_ref, 32 * layer, W1, H1), sc_ref[6 + layer:7 + layer, :1])
                nv_ref[layer], qv_ref[layer] = lars_block(v_ref[layer], pv_ref[layer], get_units(gv_ref, 32 * layer, H1, W1), sc_ref[8 + layer:9 + layer, :1])
            nm_ref[...], qm_ref[...] = lars_block(m_ref[...], pm_ref[...], get_units(gm_ref, 0, W2, W2), sc_ref[4:5, :1])
            ub_ref[...] = halve(nu_ref[...])
            vb_ref[...] = nv_ref[...].astype(BF16)
            mb_ref[...] = nm_ref[...].astype(BF16)

        res_ref[...] = stage_one_tile(token_parts(x_ref, x_s), ub_ref, vb_ref, mb_ref)[2]

    shapes = ONE_SHAPES
    units = [pl.BlockSpec((size, 16, 128), lambda i, at=at: (at, 0, 0)) for size, at in ((64, 38), (64, 39), (128, 16))]
    return pl.pallas_call(
        kernel,
        grid=(NT,),
        in_specs=[whole(SCALE_SHAPE), rows_spec(TOKENS, W1)] + [whole(s) for s in shapes] * 2 + units,
        out_specs=[rows_spec(TILE, W2)] + [whole(s) for s in shapes] * 2,
        out_shape=[struct((ROWS, W2), BF16)] + [struct(s, F32) for s in shapes] * 2,
        scratch_shapes=[pltpu.VMEM(s, BF16) for s in shapes] + [pltpu.VMEM((TOKENS, W1), F32)],
        compiler_params=params(),
        name="stage_one_next",
    )(scales, x, *weights, *vels, grads, grads, grads)


def row_parts():
    return [(sum(SPLITS[:index]), size) for index, size in enumerate(SPLITS)]


def stage_two_start(chunk, src_ref, dst_norm, acc_ref):
    for start, size in row_parts():
        resid = src_ref[start:start + size].astype(F32)
        dst_norm[start:start + size] = ln_parts(resid)[0].astype(BF16)
        acc_ref[start:start + size] = resid


def stage_two_step(norm_ref, acc_ref, ub, vb):
    for start, size in row_parts():
        act = gelu_fwd(dot_nn(norm_ref[start:start + size], ub)).astype(BF16)
        acc_ref[start:start + size] += dot_nn(act, vb)


def pool_images(resid_ref):
    cols = lax.broadcasted_iota(jnp.int32, (16, ROWS_PAD), 1)
    base = lax.broadcasted_iota(jnp.int32, (16, ROWS_PAD), 0) * PER_IMAGE
    mask = ((cols >= base) & (cols < base + PER_IMAGE) & (cols < ROWS)).astype(F32).astype(BF16)
    return dot_nn(mask, resid_ref[...]) * (1.0 / PER_IMAGE)


def head_block(layer, chunk, h_ref, classes):
    at = pl.multiple_of((layer * NF + chunk) * HEAD_ROWS, HEAD_ROWS)
    rows = at + lax.broadcasted_iota(jnp.int32, h_ref.shape, 0)
    return at, jnp.where(rows < classes, h_ref[...], 0.0)


def two_specs():
    u_spec = pl.BlockSpec((1, W2, FCHUNK), lambda l, j: (l, 0, j))
    v_spec = pl.BlockSpec((1, FCHUNK, W2), lambda l, j: (l, j, 0))
    return u_spec, v_spec, pl.BlockSpec((HEAD_ROWS, W2), lambda l, j: (l * NF + j, 0))


def by_layer(layer, chunk):
    return layer, 0, 0


def stage_two_now(res_in, labels, up_two, down_two, head, global_batch):
    classes = head.shape[0]
    images = labels.shape[0]

    def kernel(r_ref, lab_ref, u_ref, v_ref, h_ref, mid_ref, ub_ref, vb_ref, su_ref, sv_ref, sh_ref, dh_ref, gp_ref, norm_s, acc_s, res_s, hb_s):
        layer, chunk = pl.program_id(0), pl.program_id(1)

        @pl.when((layer == 0) & (chunk == 0))
        def _():
            sh_ref[...] = jnp.zeros_like(sh_ref)

        @pl.when(chunk == 0)
        def _():
            @pl.when(layer == 0)
            def _():
                stage_two_start(chunk, r_ref, norm_s, acc_s)

            @pl.when(layer == 1)
            def _():
                stage_two_start(chunk, mid_ref, norm_s, acc_s)
            su_ref[...] = jnp.zeros_like(su_ref)
            sv_ref[...] = jnp.zeros_like(sv_ref)

        ub = halve(u_ref[0])
        vb = v_ref[0].astype(BF16)
        ub_ref[0] = ub
        vb_ref[0] = halve(v_ref[0])
        su_ref[0] += fold_sq(u_ref[0])
        sv_ref[0] += fold_sq(v_ref[0])
        at, head_part = head_block(layer, chunk, h_ref, classes)
        sh_ref[...] += fold_sq(head_part)
        hb_s[pl.ds(at, HEAD_ROWS)] = head_part.astype(BF16)
        stage_two_step(norm_s, acc_s, ub, vb)

        @pl.when((chunk == NF - 1) & (layer == 0))
        def _():
            mid_ref[...] = acc_s[...].astype(BF16)

        @pl.when((chunk == NF - 1) & (layer == 1))
        def _():
            res_s[:ROWS] = acc_s[...].astype(BF16)
            res_s[ROWS:] = jnp.zeros((ROWS_PAD - ROWS, W2), BF16)
            normed, inv = ln_parts(pool_images(res_s))
            head_in = normed.astype(BF16)
            logits = dot_nt(head_in, hb_s[...])
            cols = lax.broadcasted_iota(jnp.int32, logits.shape, 1)
            rows = lax.broadcasted_iota(jnp.int32, logits.shape, 0)
            live = cols < classes
            top = jnp.max(jnp.where(live, logits, -jnp.inf), axis=-1, keepdims=True)
            expd = jnp.where(live, jnp.exp(logits - top), 0.0)
            probs = expd / jnp.sum(expd, axis=-1, keepdims=True)
            onehot = (cols == lab_ref[...]).astype(F32)
            grad_logits = jnp.where(rows < images, (probs - onehot) / global_batch, 0.0).astype(BF16)
            grad_head = dot_tn(grad_logits, head_in).astype(BF16)
            for block in range(2 * NF):
                put_units(dh_ref, block * HEAD_UNITS, grad_head[block * HEAD_ROWS:(block + 1) * HEAD_ROWS])
            grad_pool = ln_back(normed, inv, dot_nn(grad_logits, hb_s[...])) / PER_IMAGE
            gp_ref[...] = jnp.zeros_like(gp_ref)
            gp_ref[:16] = grad_pool.astype(BF16)

    u_spec, v_spec, h_spec = two_specs()
    return pl.pallas_call(
        kernel,
        grid=(2, NF),
        in_specs=[whole((ROWS, W2)), whole((16, 1)), u_spec, v_spec, h_spec],
        out_specs=[whole((ROWS, W2)), u_spec, v_spec, pl.BlockSpec((1, 8, FCHUNK), by_layer), pl.BlockSpec((1, 8, W2), by_layer), whole((8, W2)), whole((256, UNIT, LANES)), whole((LANES, W2))],
        out_shape=[struct((ROWS, W2), BF16), struct(UP_SHAPE, BF16), struct(DOWN_SHAPE, BF16), struct((2, 8, FCHUNK), F32), struct((2, 8, W2), F32), struct((8, W2), F32), unit_struct(256), struct((LANES, W2), BF16)],
        scratch_shapes=[pltpu.VMEM((ROWS, W2), BF16), pltpu.VMEM((ROWS, W2), F32), pltpu.VMEM((ROWS_PAD, W2), BF16), pltpu.VMEM((HEAD_PAD, W2), BF16)],
        compiler_params=params(),
        name="stage_two_now",
    )(res_in, jnp.pad(labels, (0, 16 - images))[:, None], up_two, down_two, head)


def stage_two_next(res_in, scales, grads, weights, vels, images):
    classes = weights[2].shape[0]

    def kernel(sc_ref, r_ref, u_ref, v_ref, h_ref, pu_ref, pv_ref, ph_ref, gu_ref, gv_ref, gh_ref, nu_ref, nv_ref, nh_ref, qu_ref, qv_ref, qh_ref, out_ref, norm_s, acc_s, res_s, hb_s):
        layer, chunk = pl.program_id(0), pl.program_id(1)

        @pl.when(chunk == 0)
        def _():
            @pl.when(layer == 0)
            def _():
                stage_two_start(chunk, r_ref, norm_s, acc_s)

            @pl.when(layer == 1)
            def _():
                stage_two_start(chunk, res_s, norm_s, acc_s)

        new_u, qu_ref[0] = lars_block(u_ref[0], pu_ref[0], get_units(gu_ref, 0, W2, FCHUNK), sc_ref[pl.ds(layer, 1), :1])
        nu_ref[0] = new_u
        for part in range(FCHUNK // CHUNK):
            rows = slice(part * CHUNK, (part + 1) * CHUNK)
            nv_ref[0, rows], qv_ref[0, rows] = lars_block(v_ref[0, rows], pv_ref[0, rows], get_units(gv_ref, part * CHUNK_UNITS, CHUNK, W2), sc_ref[pl.ds(2 + layer, 1), :1])
        nh_ref[...], qh_ref[...] = lars_block(h_ref[...], ph_ref[...], get_units(gh_ref, 0, HEAD_ROWS, W2), sc_ref[5:6, :1])
        at, head_part = head_block(layer, chunk, nh_ref, classes)
        hb_s[pl.ds(at, HEAD_ROWS)] = head_part.astype(BF16)
        stage_two_step(norm_s, acc_s, halve(new_u), nv_ref[0].astype(BF16))

        @pl.when(chunk == NF - 1)
        def _():
            res_s[:ROWS] = acc_s[...].astype(BF16)

            @pl.when(layer == 1)
            def _():
                res_s[ROWS:] = jnp.zeros((ROWS_PAD - ROWS, W2), BF16)
                head_in = ln_parts(pool_images(res_s))[0].astype(BF16)
                out_ref[...] = dot_nt(head_in, hb_s[...])[:images, :classes]

    u_spec, v_spec, h_spec = two_specs()
    units = [pl.BlockSpec((size, UNIT, LANES), lambda l, j, base=base // size: (base + l * NF + j, 0, 0)) for size, base in ((F_UNITS, 0), (F_UNITS, 1024), (HEAD_UNITS, 2176))]
    return pl.pallas_call(
        kernel,
        grid=(2, NF),
        in_specs=[whole(SCALE_SHAPE), whole((ROWS, W2))] + [u_spec, v_spec, h_spec] * 2 + units,
        out_specs=[u_spec, v_spec, h_spec] * 2 + [whole((images, classes))],
        out_shape=[struct(UP_SHAPE, F32), struct(DOWN_SHAPE, F32), struct((classes, W2), F32)] * 2 + [struct((images, classes), F32)],
        scratch_shapes=[pltpu.VMEM((ROWS, W2), BF16), pltpu.VMEM((ROWS, W2), F32), pltpu.VMEM((ROWS_PAD, W2), BF16), pltpu.VMEM((HEAD_PAD, W2), BF16)],
        compiler_params=params(),
        name="stage_two_next",
    )(scales, res_in, *weights, *vels, grads, grads, grads)


def stage_two_back(grad_pool, res_in, res_mid, merged, up_b, down_b, merge_b):
    def kernel(gp_ref, r0_ref, r1_ref, m_ref, u_ref, v_ref, mw_ref, du_ref, dv_ref, dm_ref, gout_ref, g_s, gt_s, n_s, nt_s, act_s, pre_s, dn_s):
        step, chunk = pl.program_id(0), pl.program_id(1)

        @pl.when((step == 0) & (chunk == 0))
        def _():
            rows = lax.broadcasted_iota(jnp.int32, (ROWS, 128), 0)
            base = lax.broadcasted_iota(jnp.int32, (ROWS, 128), 1) * PER_IMAGE
            mask = ((rows >= base) & (rows < base + PER_IMAGE)).astype(F32).astype(BF16)
            g_s[...] = dot_nn(mask, gp_ref[...]).astype(BF16)
            gt_s[...] = jnp.zeros_like(gt_s)
            nt_s[...] = jnp.zeros_like(nt_s)
            gt_s[:, :ROWS] = g_s[...].T
            act_s[ROWS:] = jnp.zeros((ROWS_PAD - ROWS, CHUNK), BF16)
            pre_s[ROWS:] = jnp.zeros((ROWS_PAD - ROWS, CHUNK), BF16)

        def begin(src_ref):
            n_s[...] = ln_parts(src_ref[...].astype(F32))[0].astype(BF16)
            nt_s[:, :ROWS] = n_s[...].T
            dn_s[...] = jnp.zeros_like(dn_s)

        @pl.when((step == 0) & (chunk == 0))
        def _():
            begin(r1_ref)

        @pl.when((step == 1) & (chunk == 0))
        def _():
            begin(r0_ref)

        ub = u_ref[0]
        vb = v_ref[0]
        for start, size in row_parts():
            act, slope = gelu_both(dot_nn(n_s[start:start + size], ub))
            grad_pre = (dot_nt(g_s[start:start + size], vb) * slope).astype(BF16)
            act_s[start:start + size] = act.astype(BF16)
            pre_s[start:start + size] = grad_pre
            dn_s[start:start + size] += dot_nt(grad_pre, ub)
        put_units(du_ref, 0, dot_nn(nt_s[...], pre_s[...]).astype(BF16))
        put_units(dv_ref, 0, dot_nn(gt_s[...], act_s[...]).T.astype(BF16))

        def finish(src_ref):
            normed, inv = ln_parts(src_ref[...].astype(F32))
            g_s[...] = (ln_back(normed, inv + inv, dn_s[...]) + g_s[...].astype(F32)).astype(BF16)

        @pl.when((step == 0) & (chunk == NCH - 1))
        def _():
            finish(r1_ref)
            gt_s[:, :ROWS] = g_s[...].T

        @pl.when((step == 1) & (chunk == NCH - 1))
        def _():
            finish(r0_ref)
            gout_ref[...] = dot_nt(g_s[...], mw_ref[...]).astype(BF16)
            put_units(dm_ref, 0, dot_tn(m_ref[...], g_s[...]).astype(BF16))

    u_spec = pl.BlockSpec((1, W2, CHUNK), lambda l, j: (1 - l, 0, j))
    v_spec = pl.BlockSpec((1, CHUNK, W2), lambda l, j: (1 - l, j, 0))
    g_spec = pl.BlockSpec((CHUNK_UNITS, UNIT, LANES), lambda l, j: ((1 - l) * NCH + j, 0, 0))
    act = whole((ROWS, W2))
    return pl.pallas_call(
        kernel,
        grid=(2, NCH),
        in_specs=[whole((128, W2)), act, act, act, u_spec, v_spec, whole((W2, W2))],
        out_specs=[g_spec, g_spec, whole((128, UNIT, LANES)), act],
        out_shape=[unit_struct(1024), unit_struct(1024), unit_struct(128), struct((ROWS, W2), BF16)],
        scratch_shapes=[pltpu.VMEM((ROWS, W2), BF16), pltpu.VMEM((W2, ROWS_PAD), BF16), pltpu.VMEM((ROWS, W2), BF16), pltpu.VMEM((W2, ROWS_PAD), BF16), pltpu.VMEM((ROWS_PAD, CHUNK), BF16), pltpu.VMEM((ROWS_PAD, CHUNK), BF16), pltpu.VMEM((ROWS, W2), F32)],
        compiler_params=params(),
        name="stage_two_back",
    )(grad_pool, res_in, res_mid, merged, up_b, down_b, merge_b)


def stage_one_back(grad_in, x, mid, up_b, down_b):
    def kernel(g_ref, x_ref, mid_ref, u_ref, v_ref, du_ref, dv_ref, du_s, dv_s, x_s, vh_s):
        tile_id = pl.program_id(0)

        @pl.when(tile_id == 0)
        def _():
            du_s[...] = jnp.zeros_like(du_s)
            dv_s[...] = jnp.zeros_like(dv_s)
            vh_s[...] = halve(v_ref[...].astype(F32))

        for quarter, start in enumerate(token_parts(x_ref, x_s)):
            cols = slice(quarter * W1, (quarter + 1) * W1)
            grad = g_ref[:, cols]
            for layer in (1, 0):
                normed, inv = ln_parts(mid_ref[:, cols].astype(F32) if layer else start)
                normed_b = normed.astype(BF16)
                act, slope = gelu_both(dot_nn(normed_b, u_ref[layer]))
                grad_pre = (dot_nt(grad, vh_s[layer]) * slope).astype(BF16)
                du_s[layer] += dot_tn(normed_b, grad_pre)
                dv_s[layer] += dot_tn(grad, act.astype(BF16))
                if layer:
                    grad_norm = dot_nt(grad_pre, u_ref[layer])
                    grad = (ln_back(normed, inv + inv, grad_norm) + grad.astype(F32)).astype(BF16)

        @pl.when(tile_id == NT - 1)
        def _():
            for layer in range(2):
                put_units(du_ref, 32 * layer, du_s[layer].astype(BF16))
                put_units(dv_ref, 32 * layer, dv_s[layer].T.astype(BF16))

    tile = rows_spec(TILE, W2)
    return pl.pallas_call(
        kernel,
        grid=(NT,),
        in_specs=[tile, rows_spec(TOKENS, W1), tile] + [whole(s) for s in ONE_SHAPES[:2]],
        out_specs=[whole((64, UNIT, LANES))] * 2,
        out_shape=[unit_struct(64)] * 2,
        scratch_shapes=[pltpu.VMEM(ONE_SHAPES[0], F32), pltpu.VMEM(ONE_SHAPES[0], F32), pltpu.VMEM((TOKENS, W1), F32), pltpu.VMEM(ONE_SHAPES[1], BF16)],
        compiler_params=params(),
        name="stage_one_back",
    )(grad_in, x, mid, up_b, down_b)


AXIS_STEP = (2, 8, 32)
STREAM_UNITS = (14, 14, 13, 13, 13, 13)
HALF = 1280
TOTAL = 2 * HALF
COUNTS = (512,) * 4 + (128, 256) + (32,) * 4
SEGMENTS = (1024, 1024, 128, 256, 64, 64)


def stream_plan():
    plan, base, slot = [], 0, 0
    for index, units in enumerate(STREAM_UNITS):
        order, sub = index // 2, index % 2
        axes = [(order + shift) % 3 for shift in range(3)]
        hops = [(axis, (sub + turn) % 2) for axis in axes for turn in range(2)]
        plan.append((units, base, slot, hops))
        base += 16 * units
        slot += 17 * units
    return plan, slot


def sum_grads(parts, squares):
    plan, slot_units = stream_plan()
    count = len(plan)

    def kernel(*refs):
        part_refs, sq_refs = refs[:6], refs[6:12]
        out_ref, scale_ref, flat, pair_buf, slots, load_sem, out_sem, pair_send, pair_recv, back_send, back_recv, hop_send, hop_recv, ready = refs[12:]
        me = lax.axis_index('data')
        core = lax.rem(me, 2)
        peer = me + 1 - 2 * core
        mine = core * HALF
        theirs = (1 - core) * HALF
        spots = [lax.rem(me // step, 4) for step in AXIS_STEP]
        partner, bit = {}, {}
        for axis in range(3):
            spot = spots[axis]
            partner[axis, 0] = me + (1 - 2 * lax.rem(spot, 2)) * AXIS_STEP[axis]
            partner[axis, 1] = me + (3 - 2 * spot) * AXIS_STEP[axis]
            bit[axis, 0] = lax.rem((spot + 1) // 2, 2)
            bit[axis, 1] = spot // 2

        loads = [pltpu.make_async_copy(part_refs[k], flat.at[pl.ds(sum(SEGMENTS[:k]), size)], load_sem.at[k]) for k, size in enumerate(SEGMENTS)]
        for load in loads:
            load.start()
        barrier = pltpu.get_barrier_semaphore()
        for other in [peer] + list(partner.values()):
            pl.semaphore_signal(barrier, inc=1, device_id=(other,), device_id_type=pl.DeviceIdType.MESH)
        pl.semaphore_wait(barrier, 7)
        for load in loads:
            load.wait()

        def send(src, dst, send_sem, recv_sem, device):
            copy = pltpu.make_async_remote_copy(src_ref=src, dst_ref=dst, send_sem=send_sem, recv_sem=recv_sem, device_id=(device,), device_id_type=pl.DeviceIdType.MESH)
            copy.start()
            return copy

        def add_in(start, src, src_start, units, blocks):
            def body(index, carry):
                at = pl.ds(start + index * units, units)
                flat[at] = flat[at] + src[pl.ds(src_start + index * units, units)]
                return carry
            lax.fori_loop(0, blocks, body, 0)

        pairs = [send(flat.at[pl.ds(theirs + base, 16 * units)], pair_buf.at[pl.ds(base, 16 * units)], pair_send.at[k], pair_recv.at[k], peer) for k, (units, base, slot, hops) in enumerate(plan)]
        held = [mine + base for units, base, slot, hops in plan]
        kept, gone = [[] for _ in plan], [[] for _ in plan]
        for k, (units, base, slot, hops) in enumerate(plan):
            start = held[k]
            for turn in range(4):
                size = (8 >> turn) * units
                flag = bit[hops[turn]]
                gone[k].append(start + (1 - flag) * size)
                start = start + flag * size
                kept[k].append(start)
        copies = {}

        def slot_at(k, turn):
            units, slot = plan[k][0], plan[k][2]
            return slot + sum((8 >> t) if t < 4 else 1 for t in range(turn)) * units

        def hop(k, turn):
            units, hops = plan[k][0], plan[k][3]
            size = (8 >> turn) * units if turn < 4 else units
            src = gone[k][turn] if turn < 4 else kept[k][3]
            copies[k, turn] = send(flat.at[pl.ds(src, size)], slots.at[pl.ds(slot_at(k, turn), size)], hop_send.at[k, turn], hop_recv.at[k, turn], partner[hops[turn]])

        for k in range(count):
            units, base = plan[k][:2]
            pairs[k].wait_recv()
            add_in(gone[k][0], pair_buf, gone[k][0] - mine, units, 8)
            hop(k, 0)
            add_in(kept[k][0], pair_buf, kept[k][0] - mine, units, 8)
        def tell(k, turn, device):
            pl.semaphore_signal(ready.at[k, turn], inc=1, device_id=(device,), device_id_type=pl.DeviceIdType.MESH)

        for turn in range(6):
            if turn == 5:
                for k in range(count):
                    pairs[k].wait_send()
                    tell(k, 4, peer)
                    for early in range(4):
                        copies[k, early].wait_send()
                        tell(k, early, partner[plan[k][3][early]])
            for k in range(count):
                units = plan[k][0]
                copies[k, turn].wait_recv()
                if turn < 3:
                    blocks = 4 >> turn
                    for dst in (gone[k][turn + 1], kept[k][turn + 1]):
                        add_in(dst, slots, slot_at(k, turn) + dst - kept[k][turn], units, blocks)
                        if dst is gone[k][turn + 1]:
                            hop(k, turn + 1)
                else:
                    if turn > 3:
                        copies[k, turn].wait_send()
                    add_in(kept[k][3], slots, slot_at(k, turn), units, 1)
                    if turn < 5:
                        hop(k, turn + 1)
        outs = []

        def share(k, turn):
            units, hops = plan[k][0], plan[k][3]
            region = pl.ds(kept[k][turn], (8 >> turn) * units)
            pl.semaphore_wait(ready.at[k, turn], 1)
            copies[k, 9 - turn] = send(flat.at[region], flat.at[region], hop_send.at[k, 9 - turn], hop_recv.at[k, 9 - turn], partner[hops[turn]])

        def put(region, index):
            copy = pltpu.make_async_copy(flat.at[region], out_ref.at[region], out_sem.at[index])
            copy.start()
            outs.append(copy)

        backs = {}
        for k in range(count):
            share(k, 3)
        for turn in (3, 2, 1, 0):
            for k in range(count):
                units = plan[k][0]
                copies[k, 9 - turn].wait_recv()
                if turn:
                    share(k, turn - 1)
                if turn < 2:
                    region = pl.ds(kept[k][0] if turn else gone[k][0], 8 * units)
                    if turn:
                        pl.semaphore_wait(ready.at[k, 4], 1)
                    backs[k, turn] = send(flat.at[region], flat.at[region], back_send.at[k, turn], back_recv.at[k, turn], peer)
                    put(region, 4 * k + turn)
        for k in range(count):
            for turn in (1, 0):
                backs[k, turn].wait_recv()
            put(pl.ds(theirs + plan[k][1], 16 * plan[k][0]), 4 * k + 2)
        squares = [ref.at[row] for ref in sq_refs for row in range(ref.shape[0])]
        for index, size in enumerate(COUNTS):
            def body(step, total, first=sum(COUNTS[:index])):
                block = flat[pl.ds(first + step * UNIT, UNIT)].astype(F32)
                return total + jnp.sum(block * block, axis=HERE_AXES, keepdims=True)[0]
            grad_sq = jnp.sum(lax.fori_loop(0, size // UNIT, body, jnp.zeros((1, LANES), F32)), axis=-1, keepdims=True)
            weight_sq = jnp.sum(jnp.sum(squares[index][...], axis=0, keepdims=True), axis=-1, keepdims=True)
            scale_ref[pl.ds(index, 1), :] = jnp.broadcast_to(TRUST * (jnp.sqrt(weight_sq) / jnp.sqrt(grad_sq)), (1, LANES))
        for copy in outs:
            copy.wait()
        for k in range(count):
            for turn in (1, 0):
                backs[k, turn].wait_send()
            for turn in range(6, 10):
                copies[k, turn].wait_send()

    anywhere = pl.BlockSpec(memory_space=pl.ANY)
    vmem = pl.BlockSpec(memory_space=pltpu.VMEM)
    dma = pltpu.SemaphoreType.DMA
    return pl.pallas_call(
        kernel,
        in_specs=[anywhere] * 6 + [vmem] * 6,
        out_specs=[anywhere, vmem],
        out_shape=[unit_struct(TOTAL), struct(SCALE_SHAPE, F32)],
        scratch_shapes=[pltpu.VMEM((TOTAL, UNIT, LANES), BF16), pltpu.VMEM((HALF, UNIT, LANES), BF16), pltpu.VMEM((slot_units, UNIT, LANES), BF16), dma((6,)), dma((4 * count,)), dma((count,)), dma((count,)), dma((count, 2)), dma((count, 2)), dma((count, 10)), dma((count, 10)), pltpu.SemaphoreType.REGULAR((count, 5))],
        compiler_params=params(collective_id=0, has_side_effects=True),
        name="sum_grads",
    )(*parts, *squares)


def solution(mesh):
    data_devs = mesh.shape['data']

    def local_step(x_now, labels_now, x_next, up_one, down_one, merge_proj, up_two, down_two, head_proj, vel_up_one, vel_down_one, vel_merge_proj, vel_up_two, vel_down_two, vel_head_proj):
        images = x_now.shape[0]
        xn = x_now.reshape(4 * ROWS, W1)
        xf = x_next.reshape(4 * ROWS, W1)
        mid, merged, res0, ub1, vb1, mb, su1, sv1, sm = stage_one_now(xn, up_one, down_one, merge_proj)
        res1, ub2, vb2, su2, sv2, sh, dh, grad_pool = stage_two_now(res0, labels_now, up_two, down_two, head_proj.T, images * data_devs)
        du2, dv2, dm, grad_mid = stage_two_back(grad_pool, res0, res1, merged, ub2, vb2, mb)
        du1, dv1 = stage_one_back(grad_mid, xn, mid, ub1, vb1)
        grads, scales = sum_grads((du2, dv2, dm, dh, du1, dv1), (su2, sv2, sm[None], sh[None], su1, sv1))
        res_f, nu1, nv1, nm, qu1, qv1, qm = stage_one_next(xf, scales, grads, (up_one, down_one, merge_proj), (vel_up_one, vel_down_one, vel_merge_proj))
        nu2, nv2, nh, qu2, qv2, qh, logits = stage_two_next(res_f, scales, grads, (up_two, down_two, head_proj.T), (vel_up_two, vel_down_two, vel_head_proj.T), images)
        return logits, nu1, nv1, nm, nu2, nv2, nh.T, qu1, qv1, qm, qu2, qv2, qh.T

    batch_split = P('data')
    in_specs = (batch_split,) * 3 + (P(),) * 12
    out_specs = (batch_split,) + (P(),) * 12
    return jax.shard_map(local_step, mesh=mesh, in_specs=in_specs, out_specs=out_specs, check_vma=False)
```

```python
import functools

import jax
import jax.numpy as jnp
from jax import lax
from jax.experimental import pallas as pl
from jax.experimental.pallas import tpu as pltpu
from jax.sharding import PartitionSpec as P

MOMENTUM = 0.9
TRUST = 0.1
LN_EPS = 1e-6
GELU_A = 2.0 * 0.7978845608028654
GELU_B = 4.0 * GELU_A * 0.044715
UNIT = 16
LANES = 128
UNIT_SIZE = UNIT * LANES
ROWS = 1568
ROWS_PAD = 1792
PER_IMAGE = 196
W1 = 128
W2 = 512
H1 = 512
H2 = 2048
CHUNK = 512
NCH = H2 // CHUNK
FCHUNK = 1024
NF = H2 // FCHUNK
TILE = 784
NT = ROWS // TILE
TOKENS = 4 * TILE
SPLITS = (784, 784)
HEAD_PAD = 1024
HEAD_ROWS = HEAD_PAD // (2 * NF)
HEAD_UNITS = HEAD_ROWS * W2 // UNIT_SIZE
HERE_AXES = (0, 1)
CHUNK_UNITS = CHUNK * W2 // UNIT_SIZE
F_UNITS = FCHUNK * W2 // UNIT_SIZE
SCALE_SHAPE = (UNIT, LANES)
ONE_SHAPES = [(2, W1, H1), (2, H1, W1), (W2, W2)]
UP_SHAPE, DOWN_SHAPE = (2, W2, H2), (2, H2, W2)
VMEM_LIMIT = 63 * 1024 * 1024
F32 = jnp.float32
BF16 = jnp.bfloat16


def dot_nn(lhs, rhs):
    return lax.dot_general(lhs, rhs, (((1,), (0,)), ((), ())), preferred_element_type=F32)


def dot_nt(lhs, rhs):
    return lax.dot_general(lhs, rhs, (((1,), (1,)), ((), ())), preferred_element_type=F32)


def dot_tn(lhs, rhs):
    return lax.dot_general(lhs, rhs, (((0,), (0,)), ((), ())), preferred_element_type=F32)


def ln_parts(values):
    row_mean = jnp.mean(values, axis=-1, keepdims=True)
    centered = values - row_mean
    variance = jnp.mean(centered * centered, axis=-1, keepdims=True)
    inv = lax.rsqrt(variance + LN_EPS)
    return centered * inv, inv


def ln_back(normed, inv, grad):
    mean_grad = jnp.mean(grad, axis=-1, keepdims=True)
    mean_dot = jnp.mean(grad * normed, axis=-1, keepdims=True)
    return inv * (grad - mean_grad - normed * mean_dot)


def gelu_fwd(half):
    tan = jnp.tanh(half * (GELU_A + GELU_B * (half * half)))
    return half + half * tan


def gelu_both(half):
    sq = half * half
    tan = jnp.tanh(half * (GELU_A + GELU_B * sq))
    above = 1.0 + tan
    return half * above, above * (1.0 + (half * (1.0 - tan)) * (GELU_A + (3.0 * GELU_B) * sq))


def halve(weight):
    return (0.5 * weight).astype(BF16)


def fold_sq(mat):
    rows, cols = mat.shape
    return jnp.sum((mat * mat).reshape(rows // 8, 8, cols), axis=0)


def lars_block(weight, vel, grad, scale):
    new_vel = MOMENTUM * vel + scale * grad.astype(F32)
    return weight - new_vel, new_vel


def put_units(ref, start, mat):
    rows, cols = mat.shape
    groups = rows // UNIT
    for lane in range(cols // LANES):
        ref[pl.ds(start + lane * groups, groups)] = mat[:, lane * LANES:(lane + 1) * LANES].reshape(groups, UNIT, LANES)


def get_units(ref, start, rows, cols):
    groups = rows // UNIT
    parts = [ref[pl.ds(start + lane * groups, groups)].reshape(rows, LANES) for lane in range(cols // LANES)]
    return parts[0] if len(parts) == 1 else jnp.concatenate(parts, axis=1)


struct = jax.ShapeDtypeStruct


def unit_struct(count):
    return struct((count, UNIT, LANES), BF16)


def params(**kwargs):
    return pltpu.CompilerParams(vmem_limit_bytes=VMEM_LIMIT, **kwargs)


def whole(shape):
    zeros = (0,) * len(shape)
    return pl.BlockSpec(shape, lambda *_: zeros)


def token_parts(x_ref, x_s):
    x_s[...] = x_ref[...].astype(F32)
    return [x_s[pl.ds(quarter, TILE, stride=4), :] for quarter in range(4)]


def stage_one_tile(parts, ub, vb, mb):
    outs0, outs1 = [], []
    for resid in parts:
        for layer in range(2):
            normed = ln_parts(resid.astype(F32))[0].astype(BF16)
            act = gelu_fwd(dot_nn(normed, ub[layer])).astype(BF16)
            resid = (resid.astype(F32) + dot_nn(act, vb[layer])).astype(BF16)
            (outs0, outs1)[layer].append(resid)
    mid = jnp.concatenate(outs0, axis=1)
    merged = jnp.concatenate(outs1, axis=1)
    return mid, merged, dot_nn(merged, mb[...]).astype(BF16)


def rows_spec(rows, cols):
    return pl.BlockSpec((rows, cols), lambda i: (i, 0))


def stage_one_now(x, up_one, down_one, merge):
    def kernel(x_ref, u_ref, v_ref, m_ref, mid_ref, merged_ref, res_ref, ub_ref, vb_ref, mb_ref, su_ref, sv_ref, sm_ref, x_s):
        @pl.when(pl.program_id(0) == 0)
        def _():
            ub_ref[...] = halve(u_ref[...])
            vb_ref[...] = v_ref[...].astype(BF16)
            mb_ref[...] = m_ref[...].astype(BF16)
            for layer in range(2):
                su_ref[layer] = fold_sq(u_ref[layer])
                sv_ref[layer] = fold_sq(v_ref[layer])
            sm_ref[...] = fold_sq(m_ref[...])

        mid, merged, res = stage_one_tile(token_parts(x_ref, x_s), ub_ref, vb_ref, mb_ref)
        mid_ref[...] = mid
        merged_ref[...] = merged
        res_ref[...] = res

    tile = rows_spec(TILE, W2)
    act = struct((ROWS, W2), BF16)
    small = [(shape, BF16) for shape in ONE_SHAPES] + [((2, 8, H1), F32), ((2, 8, W1), F32), ((8, W2), F32)]
    return pl.pallas_call(
        kernel,
        grid=(NT,),
        in_specs=[rows_spec(TOKENS, W1)] + [whole(s) for s in ONE_SHAPES],
        out_specs=[tile] * 3 + [whole(s) for s, _ in small],
        out_shape=[act] * 3 + [struct(s, d) for s, d in small],
        scratch_shapes=[pltpu.VMEM((TOKENS, W1), F32)],
        compiler_params=params(),
        name="stage_one_now",
    )(x, up_one, down_one, merge)


def stage_one_next(x, scales, grads, weights, vels):
    def kernel(sc_ref, x_ref, u_ref, v_ref, m_ref, pu_ref, pv_ref, pm_ref, gu_ref, gv_ref, gm_ref, res_ref, nu_ref, nv_ref, nm_ref, qu_ref, qv_ref, qm_ref, ub_ref, vb_ref, mb_ref, x_s):
        @pl.when(pl.program_id(0) == 0)
        def _():
            for layer in range(2):
                nu_ref[layer], qu_ref[layer] = lars_block(u_ref[layer], pu_ref[layer], get_units(gu_ref, 32 * layer, W1, H1), sc_ref[6 + layer:7 + layer, :1])
                nv_ref[layer], qv_ref[layer] = lars_block(v_ref[layer], pv_ref[layer], get_units(gv_ref, 32 * layer, H1, W1), sc_ref[8 + layer:9 + layer, :1])
            nm_ref[...], qm_ref[...] = lars_block(m_ref[...], pm_ref[...], get_units(gm_ref, 0, W2, W2), sc_ref[4:5, :1])
            ub_ref[...] = halve(nu_ref[...])
            vb_ref[...] = nv_ref[...].astype(BF16)
            mb_ref[...] = nm_ref[...].astype(BF16)

        res_ref[...] = stage_one_tile(token_parts(x_ref, x_s), ub_ref, vb_ref, mb_ref)[2]

    shapes = ONE_SHAPES
    units = [pl.BlockSpec((size, 16, 128), lambda i, at=at: (at, 0, 0)) for size, at in ((64, 38), (64, 39), (128, 16))]
    return pl.pallas_call(
        kernel,
        grid=(NT,),
        in_specs=[whole(SCALE_SHAPE), rows_spec(TOKENS, W1)] + [whole(s) for s in shapes] * 2 + units,
        out_specs=[rows_spec(TILE, W2)] + [whole(s) for s in shapes] * 2,
        out_shape=[struct((ROWS, W2), BF16)] + [struct(s, F32) for s in shapes] * 2,
        scratch_shapes=[pltpu.VMEM(s, BF16) for s in shapes] + [pltpu.VMEM((TOKENS, W1), F32)],
        compiler_params=params(),
        name="stage_one_next",
    )(scales, x, *weights, *vels, grads, grads, grads)


def row_parts():
    return [(sum(SPLITS[:index]), size) for index, size in enumerate(SPLITS)]


def stage_two_start(chunk, src_ref, dst_norm, acc_ref):
    for start, size in row_parts():
        resid = src_ref[start:start + size].astype(F32)
        dst_norm[start:start + size] = ln_parts(resid)[0].astype(BF16)
        acc_ref[start:start + size] = resid


def stage_two_step(norm_ref, acc_ref, ub, vb):
    for start, size in row_parts():
        act = gelu_fwd(dot_nn(norm_ref[start:start + size], ub)).astype(BF16)
        acc_ref[start:start + size] += dot_nn(act, vb)


def pool_images(resid_ref):
    cols = lax.broadcasted_iota(jnp.int32, (16, ROWS_PAD), 1)
    base = lax.broadcasted_iota(jnp.int32, (16, ROWS_PAD), 0) * PER_IMAGE
    mask = ((cols >= base) & (cols < base + PER_IMAGE) & (cols < ROWS)).astype(F32).astype(BF16)
    return dot_nn(mask, resid_ref[...]) * (1.0 / PER_IMAGE)


def head_block(layer, chunk, h_ref, classes):
    at = pl.multiple_of((layer * NF + chunk) * HEAD_ROWS, HEAD_ROWS)
    rows = at + lax.broadcasted_iota(jnp.int32, h_ref.shape, 0)
    return at, jnp.where(rows < classes, h_ref[...], 0.0)


def two_specs():
    u_spec = pl.BlockSpec((1, W2, FCHUNK), lambda l, j: (l, 0, j))
    v_spec = pl.BlockSpec((1, FCHUNK, W2), lambda l, j: (l, j, 0))
    return u_spec, v_spec, pl.BlockSpec((HEAD_ROWS, W2), lambda l, j: (l * NF + j, 0))


def by_layer(layer, chunk):
    return layer, 0, 0


def stage_two_now(res_in, labels, up_two, down_two, head, global_batch):
    classes = head.shape[0]
    images = labels.shape[0]

    def kernel(r_ref, lab_ref, u_ref, v_ref, h_ref, mid_ref, ub_ref, vb_ref, su_ref, sv_ref, sh_ref, dh_ref, gp_ref, norm_s, acc_s, res_s, hb_s):
        layer, chunk = pl.program_id(0), pl.program_id(1)

        @pl.when((layer == 0) & (chunk == 0))
        def _():
            sh_ref[...] = jnp.zeros_like(sh_ref)

        @pl.when(chunk == 0)
        def _():
            @pl.when(layer == 0)
            def _():
                stage_two_start(chunk, r_ref, norm_s, acc_s)

            @pl.when(layer == 1)
            def _():
                stage_two_start(chunk, mid_ref, norm_s, acc_s)
            su_ref[...] = jnp.zeros_like(su_ref)
            sv_ref[...] = jnp.zeros_like(sv_ref)

        ub = halve(u_ref[0])
        vb = v_ref[0].astype(BF16)
        ub_ref[0] = ub
        vb_ref[0] = halve(v_ref[0])
        su_ref[0] += fold_sq(u_ref[0])
        sv_ref[0] += fold_sq(v_ref[0])
        at, head_part = head_block(layer, chunk, h_ref, classes)
        sh_ref[...] += fold_sq(head_part)
        hb_s[pl.ds(at, HEAD_ROWS)] = head_part.astype(BF16)
        stage_two_step(norm_s, acc_s, ub, vb)

        @pl.when((chunk == NF - 1) & (layer == 0))
        def _():
            mid_ref[...] = acc_s[...].astype(BF16)

        @pl.when((chunk == NF - 1) & (layer == 1))
        def _():
            res_s[:ROWS] = acc_s[...].astype(BF16)
            res_s[ROWS:] = jnp.zeros((ROWS_PAD - ROWS, W2), BF16)
            normed, inv = ln_parts(pool_images(res_s))
            head_in = normed.astype(BF16)
            logits = dot_nt(head_in, hb_s[...])
            cols = lax.broadcasted_iota(jnp.int32, logits.shape, 1)
            rows = lax.broadcasted_iota(jnp.int32, logits.shape, 0)
            live = cols < classes
            top = jnp.max(jnp.where(live, logits, -jnp.inf), axis=-1, keepdims=True)
            expd = jnp.where(live, jnp.exp(logits - top), 0.0)
            probs = expd / jnp.sum(expd, axis=-1, keepdims=True)
            onehot = (cols == lab_ref[...]).astype(F32)
            grad_logits = jnp.where(rows < images, (probs - onehot) / global_batch, 0.0).astype(BF16)
            grad_head = dot_tn(grad_logits, head_in).astype(BF16)
            for block in range(2 * NF):
                put_units(dh_ref, block * HEAD_UNITS, grad_head[block * HEAD_ROWS:(block + 1) * HEAD_ROWS])
            grad_pool = ln_back(normed, inv, dot_nn(grad_logits, hb_s[...])) / PER_IMAGE
            gp_ref[...] = jnp.zeros_like(gp_ref)
            gp_ref[:16] = grad_pool.astype(BF16)

    u_spec, v_spec, h_spec = two_specs()
    return pl.pallas_call(
        kernel,
        grid=(2, NF),
        in_specs=[whole((ROWS, W2)), whole((16, 1)), u_spec, v_spec, h_spec],
        out_specs=[whole((ROWS, W2)), u_spec, v_spec, pl.BlockSpec((1, 8, FCHUNK), by_layer), pl.BlockSpec((1, 8, W2), by_layer), whole((8, W2)), whole((256, UNIT, LANES)), whole((LANES, W2))],
        out_shape=[struct((ROWS, W2), BF16), struct(UP_SHAPE, BF16), struct(DOWN_SHAPE, BF16), struct((2, 8, FCHUNK), F32), struct((2, 8, W2), F32), struct((8, W2), F32), unit_struct(256), struct((LANES, W2), BF16)],
        scratch_shapes=[pltpu.VMEM((ROWS, W2), BF16), pltpu.VMEM((ROWS, W2), F32), pltpu.VMEM((ROWS_PAD, W2), BF16), pltpu.VMEM((HEAD_PAD, W2), BF16)],
        compiler_params=params(),
        name="stage_two_now",
    )(res_in, jnp.pad(labels, (0, 16 - images))[:, None], up_two, down_two, head)


def stage_two_next(res_in, scales, grads, weights, vels, images):
    classes = weights[2].shape[0]

    def kernel(sc_ref, r_ref, u_ref, v_ref, h_ref, pu_ref, pv_ref, ph_ref, gu_ref, gv_ref, gh_ref, nu_ref, nv_ref, nh_ref, qu_ref, qv_ref, qh_ref, out_ref, norm_s, acc_s, res_s, hb_s):
        layer, chunk = pl.program_id(0), pl.program_id(1)

        @pl.when(chunk == 0)
        def _():
            @pl.when(layer == 0)
            def _():
                stage_two_start(chunk, r_ref, norm_s, acc_s)

            @pl.when(layer == 1)
            def _():
                stage_two_start(chunk, res_s, norm_s, acc_s)

        new_u, qu_ref[0] = lars_block(u_ref[0], pu_ref[0], get_units(gu_ref, 0, W2, FCHUNK), sc_ref[pl.ds(layer, 1), :1])
        nu_ref[0] = new_u
        for part in range(FCHUNK // CHUNK):
            rows = slice(part * CHUNK, (part + 1) * CHUNK)
            nv_ref[0, rows], qv_ref[0, rows] = lars_block(v_ref[0, rows], pv_ref[0, rows], get_units(gv_ref, part * CHUNK_UNITS, CHUNK, W2), sc_ref[pl.ds(2 + layer, 1), :1])
        nh_ref[...], qh_ref[...] = lars_block(h_ref[...], ph_ref[...], get_units(gh_ref, 0, HEAD_ROWS, W2), sc_ref[5:6, :1])
        at, head_part = head_block(layer, chunk, nh_ref, classes)
        hb_s[pl.ds(at, HEAD_ROWS)] = head_part.astype(BF16)
        stage_two_step(norm_s, acc_s, halve(new_u), nv_ref[0].astype(BF16))

        @pl.when(chunk == NF - 1)
        def _():
            res_s[:ROWS] = acc_s[...].astype(BF16)

            @pl.when(layer == 1)
            def _():
                res_s[ROWS:] = jnp.zeros((ROWS_PAD - ROWS, W2), BF16)
                head_in = ln_parts(pool_images(res_s))[0].astype(BF16)
                out_ref[...] = dot_nt(head_in, hb_s[...])[:images, :classes]

    u_spec, v_spec, h_spec = two_specs()
    units = [pl.BlockSpec((size, UNIT, LANES), lambda l, j, base=base // size: (base + l * NF + j, 0, 0)) for size, base in ((F_UNITS, 0), (F_UNITS, 1024), (HEAD_UNITS, 2176))]
    return pl.pallas_call(
        kernel,
        grid=(2, NF),
        in_specs=[whole(SCALE_SHAPE), whole((ROWS, W2))] + [u_spec, v_spec, h_spec] * 2 + units,
        out_specs=[u_spec, v_spec, h_spec] * 2 + [whole((images, classes))],
        out_shape=[struct(UP_SHAPE, F32), struct(DOWN_SHAPE, F32), struct((classes, W2), F32)] * 2 + [struct((images, classes), F32)],
        scratch_shapes=[pltpu.VMEM((ROWS, W2), BF16), pltpu.VMEM((ROWS, W2), F32), pltpu.VMEM((ROWS_PAD, W2), BF16), pltpu.VMEM((HEAD_PAD, W2), BF16)],
        compiler_params=params(),
        name="stage_two_next",
    )(scales, res_in, *weights, *vels, grads, grads, grads)


def stage_two_back(grad_pool, res_in, res_mid, merged, up_b, down_b, merge_b):
    def kernel(gp_ref, r0_ref, r1_ref, m_ref, u_ref, v_ref, mw_ref, du_ref, dv_ref, dm_ref, gout_ref, g_s, gt_s, n_s, nt_s, act_s, pre_s, dn_s):
        step, chunk = pl.program_id(0), pl.program_id(1)

        @pl.when((step == 0) & (chunk == 0))
        def _():
            rows = lax.broadcasted_iota(jnp.int32, (ROWS, 128), 0)
            base = lax.broadcasted_iota(jnp.int32, (ROWS, 128), 1) * PER_IMAGE
            mask = ((rows >= base) & (rows < base + PER_IMAGE)).astype(F32).astype(BF16)
            g_s[...] = dot_nn(mask, gp_ref[...]).astype(BF16)
            gt_s[...] = jnp.zeros_like(gt_s)
            nt_s[...] = jnp.zeros_like(nt_s)
            gt_s[:, :ROWS] = g_s[...].T
            act_s[ROWS:] = jnp.zeros((ROWS_PAD - ROWS, CHUNK), BF16)
            pre_s[ROWS:] = jnp.zeros((ROWS_PAD - ROWS, CHUNK), BF16)

        def begin(src_ref):
            n_s[...] = ln_parts(src_ref[...].astype(F32))[0].astype(BF16)
            nt_s[:, :ROWS] = n_s[...].T
            dn_s[...] = jnp.zeros_like(dn_s)

        @pl.when((step == 0) & (chunk == 0))
        def _():
            begin(r1_ref)

        @pl.when((step == 1) & (chunk == 0))
        def _():
            begin(r0_ref)

        ub = u_ref[0]
        vb = v_ref[0]
        for start, size in row_parts():
            act, slope = gelu_both(dot_nn(n_s[start:start + size], ub))
            grad_pre = (dot_nt(g_s[start:start + size], vb) * slope).astype(BF16)
            act_s[start:start + size] = act.astype(BF16)
            pre_s[start:start + size] = grad_pre
            dn_s[start:start + size] += dot_nt(grad_pre, ub)
        put_units(du_ref, 0, dot_nn(nt_s[...], pre_s[...]).astype(BF16))
        put_units(dv_ref, 0, dot_nn(gt_s[...], act_s[...]).T.astype(BF16))

        def finish(src_ref):
            normed, inv = ln_parts(src_ref[...].astype(F32))
            g_s[...] = (ln_back(normed, inv + inv, dn_s[...]) + g_s[...].astype(F32)).astype(BF16)

        @pl.when((step == 0) & (chunk == NCH - 1))
        def _():
            finish(r1_ref)
            gt_s[:, :ROWS] = g_s[...].T

        @pl.when((step == 1) & (chunk == NCH - 1))
        def _():
            finish(r0_ref)
            gout_ref[...] = dot_nt(g_s[...], mw_ref[...]).astype(BF16)
            put_units(dm_ref, 0, dot_tn(m_ref[...], g_s[...]).astype(BF16))

    u_spec = pl.BlockSpec((1, W2, CHUNK), lambda l, j: (1 - l, 0, j))
    v_spec = pl.BlockSpec((1, CHUNK, W2), lambda l, j: (1 - l, j, 0))
    g_spec = pl.BlockSpec((CHUNK_UNITS, UNIT, LANES), lambda l, j: ((1 - l) * NCH + j, 0, 0))
    act = whole((ROWS, W2))
    return pl.pallas_call(
        kernel,
        grid=(2, NCH),
        in_specs=[whole((128, W2)), act, act, act, u_spec, v_spec, whole((W2, W2))],
        out_specs=[g_spec, g_spec, whole((128, UNIT, LANES)), act],
        out_shape=[unit_struct(1024), unit_struct(1024), unit_struct(128), struct((ROWS, W2), BF16)],
        scratch_shapes=[pltpu.VMEM((ROWS, W2), BF16), pltpu.VMEM((W2, ROWS_PAD), BF16), pltpu.VMEM((ROWS, W2), BF16), pltpu.VMEM((W2, ROWS_PAD), BF16), pltpu.VMEM((ROWS_PAD, CHUNK), BF16), pltpu.VMEM((ROWS_PAD, CHUNK), BF16), pltpu.VMEM((ROWS, W2), F32)],
        compiler_params=params(),
        name="stage_two_back",
    )(grad_pool, res_in, res_mid, merged, up_b, down_b, merge_b)


AXIS_STEP = (2, 8, 32)
MAIN_UNITS = (13, 13, 13, 13, 12, 12)
LATE_UNITS = (2, 2)
MAIN = tuple(range(len(MAIN_UNITS)))
LATE = tuple(range(len(MAIN_UNITS), len(MAIN_UNITS) + len(LATE_UNITS)))
MAIN_HALF = UNIT * sum(MAIN_UNITS)
LATE_HALF = UNIT * sum(LATE_UNITS)
TOTAL = 2 * (MAIN_HALF + LATE_HALF)
COUNTS = (512,) * 4 + (128, 256) + (32,) * 4
SEGMENTS = (1024, 1024, 128, 256)
LOOPS = ((0, 2), (2, 6), (6, 8))
HOPS = 6


def stream_plan():
    plan, base, slot = [], 0, 0
    for index, units in enumerate(MAIN_UNITS + LATE_UNITS):
        hops = [((index // 2 + turn // 2) % 3, (index + turn) % 2) for turn in range(HOPS)]
        plan.append((units, base, slot, hops))
        base += UNIT * units
        slot += (UNIT + 1) * units
    return plan, slot


def sum_grads(parts, acts, squares):
    plan, slot_units = stream_plan()
    count = len(plan)

    def kernel(*refs):
        refs = list(refs)
        take = lambda number: [refs.pop(0) for _ in range(number)]
        part_refs, sq_refs = take(len(parts)), take(len(squares))
        g_ref, x_ref, mid_ref, u_ref, v_ref, out_ref, scale_ref = take(7)
        flat, pair_buf, slots, x_s, vh_s, du_s, dv_s, load_sem, out_sem, pair_send, pair_recv, back_send, back_recv, hop_send, hop_recv, ready = refs
        me = lax.axis_index('data')
        core = lax.rem(me, 2)
        peer = me + 1 - 2 * core
        partner, bit = {}, {}
        for axis, step in enumerate(AXIS_STEP):
            spot = lax.rem(me // step, 4)
            partner[axis, 0] = me + (1 - 2 * lax.rem(spot, 2)) * step
            partner[axis, 1] = me + (3 - 2 * spot) * step
            bit[axis, 0] = lax.rem((spot + 1) // 2, 2)
            bit[axis, 1] = spot // 2

        loads = [pltpu.make_async_copy(part_refs[k], flat.at[pl.ds(sum(SEGMENTS[:k]), size)], load_sem.at[k]) for k, size in enumerate(SEGMENTS)]
        for load in loads:
            load.start()
        barrier = pltpu.get_barrier_semaphore()
        for other in [peer] + list(partner.values()):
            pl.semaphore_signal(barrier, inc=1, device_id=(other,), device_id_type=pl.DeviceIdType.MESH)
        x_s[...] = x_ref[...].astype(F32)
        vh_s[...] = halve(v_ref[...].astype(F32))
        du_s[...] = jnp.zeros_like(du_s)
        dv_s[...] = jnp.zeros_like(dv_s)
        pl.semaphore_wait(barrier, 1 + len(partner))
        for load in loads:
            load.wait()

        def send(src, dst, send_sem, recv_sem, device):
            copy = pltpu.make_async_remote_copy(src_ref=src, dst_ref=dst, send_sem=send_sem, recv_sem=recv_sem, device_id=(device,), device_id_type=pl.DeviceIdType.MESH)
            copy.start()
            return copy

        def add_in(start, src, src_start, units, blocks):
            def body(index, carry):
                at = pl.ds(start + index * units, units)
                flat[at] = flat[at] + src[pl.ds(src_start + index * units, units)]
                return carry
            lax.fori_loop(0, blocks, body, 0)

        def home(k, side):
            return plan[k][1] + (MAIN_HALF + side * LATE_HALF if k in LATE else side * MAIN_HALF)

        kept, gone = [[] for _ in plan], [[] for _ in plan]
        for k, (units, base, slot, hops) in enumerate(plan):
            start = home(k, core)
            for turn in range(4):
                size = (8 >> turn) * units
                flag = bit[hops[turn]]
                gone[k].append(start + (1 - flag) * size)
                start = start + flag * size
                kept[k].append(start)
        copies, pairs, backs, outs = {}, {}, {}, []

        def pair_up(streams):
            for k in streams:
                size = UNIT * plan[k][0]
                pairs[k] = send(flat.at[pl.ds(home(k, 1 - core), size)], pair_buf.at[pl.ds(plan[k][1], size)], pair_send.at[k], pair_recv.at[k], peer)

        def slot_at(k, turn):
            units, slot = plan[k][0], plan[k][2]
            return slot + sum((8 >> t) if t < 4 else 1 for t in range(turn)) * units

        def hop(k, turn):
            units, hops = plan[k][0], plan[k][3]
            size = (8 >> turn) * units if turn < 4 else units
            src = gone[k][turn] if turn < 4 else kept[k][3]
            copies[k, turn] = send(flat.at[pl.ds(src, size)], slots.at[pl.ds(slot_at(k, turn), size)], hop_send.at[k, turn], hop_recv.at[k, turn], partner[hops[turn]])

        def first_hops(streams):
            for k in streams:
                units, base = plan[k][:2]
                pairs[k].wait_recv()
                add_in(gone[k][0], pair_buf, base + gone[k][0] - home(k, core), units, 8)
                hop(k, 0)
                add_in(kept[k][0], pair_buf, base + kept[k][0] - home(k, core), units, 8)

        def tell(k, turn, device):
            pl.semaphore_signal(ready.at[k, turn], inc=1, device_id=(device,), device_id_type=pl.DeviceIdType.MESH)

        def reduce_turn(streams, turn):
            if turn == HOPS - 1:
                for k in streams:
                    pairs[k].wait_send()
                    tell(k, 4, peer)
                    for early in range(4):
                        copies[k, early].wait_send()
                        tell(k, early, partner[plan[k][3][early]])
            for k in streams:
                units = plan[k][0]
                copies[k, turn].wait_recv()
                if turn < 3:
                    blocks = 4 >> turn
                    at = slot_at(k, turn) - kept[k][turn]
                    away, stay = gone[k][turn + 1], kept[k][turn + 1]
                    add_in(away, slots, at + away, units, blocks)
                    hop(k, turn + 1)
                    add_in(stay, slots, at + stay, units, blocks)
                else:
                    if turn > 3:
                        copies[k, turn].wait_send()
                    add_in(kept[k][3], slots, slot_at(k, turn), units, 1)
                    if turn < HOPS - 1:
                        hop(k, turn + 1)
                    else:
                        share(k, 3)

        def share(k, turn):
            region = pl.ds(kept[k][turn], (8 >> turn) * plan[k][0])
            pl.semaphore_wait(ready.at[k, turn], 1)
            at = 2 * HOPS - 3 - turn
            copies[k, at] = send(flat.at[region], flat.at[region], hop_send.at[k, at], hop_recv.at[k, at], partner[plan[k][3][turn]])

        def put(region, index):
            copy = pltpu.make_async_copy(flat.at[region], out_ref.at[region], out_sem.at[index])
            copy.start()
            outs.append(copy)

        def gather_turn(streams, turn):
            for k in streams:
                copies[k, 2 * HOPS - 3 - turn].wait_recv()
                if turn:
                    share(k, turn - 1)
                if turn < 2:
                    region = pl.ds(kept[k][0] if turn else gone[k][0], 8 * plan[k][0])
                    if turn:
                        pl.semaphore_wait(ready.at[k, 4], 1)
                    backs[k, turn] = send(flat.at[region], flat.at[region], back_send.at[k, turn], back_recv.at[k, turn], peer)
                    put(region, 3 * k + turn)

        def token_block(index, carry):
            quarter, tile = lax.rem(index, 4), index // 4
            rows = pl.ds(pl.multiple_of(tile * TILE, UNIT), TILE)
            cols = pl.ds(pl.multiple_of(quarter * W1, W1), W1)
            grad = g_ref[rows, cols]
            for layer in (1, 0):
                source = mid_ref[rows, cols].astype(F32) if layer else x_s[pl.ds(tile * TOKENS + quarter, TILE, stride=4), :]
                normed, inv = ln_parts(source)
                normed_b = normed.astype(BF16)
                act, slope = gelu_both(dot_nn(normed_b, u_ref[layer]))
                grad_pre = (dot_nt(grad, vh_s[layer]) * slope).astype(BF16)
                du_s[layer] += dot_tn(normed_b, grad_pre)
                dv_s[layer] += dot_tn(grad, act.astype(BF16))
                if layer:
                    grad = (ln_back(normed, inv + inv, dot_nt(grad_pre, u_ref[layer])) + grad.astype(F32)).astype(BF16)
            return carry

        pair_up(MAIN)
        for number, (low, high) in enumerate(LOOPS):
            lax.fori_loop(low, high, token_block, 0)
            if number == 0:
                first_hops(MAIN)
            elif number == 1:
                reduce_turn(MAIN, 0)
        for layer in range(2):
            late = sum(SEGMENTS) + layer * (LATE_HALF // 2)
            put_units(flat, late, du_s[layer].astype(BF16))
            put_units(flat, late + LATE_HALF, dv_s[layer].T.astype(BF16))
        pair_up(LATE)
        reduce_turn(MAIN, 1)
        first_hops(LATE)
        for turn in range(2, HOPS):
            reduce_turn(MAIN, turn)
            reduce_turn(LATE, turn - 2)
        gather_turn(MAIN, 3)
        reduce_turn(LATE, HOPS - 2)
        gather_turn(MAIN, 2)
        reduce_turn(LATE, HOPS - 1)
        gather_turn(MAIN, 1)
        for turn in (3, 2, 1, 0):
            gather_turn(LATE, turn)
        gather_turn(MAIN, 0)
        for k in range(count):
            for turn in (1, 0):
                backs[k, turn].wait_recv()
            put(pl.ds(home(k, 1 - core), UNIT * plan[k][0]), 3 * k + 2)
        squares_list = [ref.at[row] for ref in sq_refs for row in range(ref.shape[0])]
        for index, size in enumerate(COUNTS):
            def body(step, total, first=sum(COUNTS[:index])):
                block = flat[pl.ds(first + step * UNIT, UNIT)].astype(F32)
                return total + jnp.sum(block * block, axis=HERE_AXES, keepdims=True)[0]
            grad_sq = jnp.sum(lax.fori_loop(0, size // UNIT, body, jnp.zeros((1, LANES), F32)), axis=-1, keepdims=True)
            weight_sq = jnp.sum(jnp.sum(squares_list[index][...], axis=0, keepdims=True), axis=-1, keepdims=True)
            scale_ref[pl.ds(index, 1), :] = jnp.broadcast_to(TRUST * (jnp.sqrt(weight_sq) / jnp.sqrt(grad_sq)), (1, LANES))
        for copy in outs:
            copy.wait()
        for k in range(count):
            for turn in (1, 0):
                backs[k, turn].wait_send()
            for turn in range(4):
                copies[k, HOPS + turn].wait_send()

    anywhere = pl.BlockSpec(memory_space=pl.ANY)
    vmem = pl.BlockSpec(memory_space=pltpu.VMEM)
    dma = pltpu.SemaphoreType.DMA
    units = lambda number: pltpu.VMEM((number, UNIT, LANES), BF16)
    both, each = (count, 2), (count, HOPS + 4)
    return pl.pallas_call(
        kernel,
        in_specs=[anywhere] * len(parts) + [vmem] * (len(squares) + len(acts)),
        out_specs=[anywhere, vmem],
        out_shape=[unit_struct(TOTAL), struct(SCALE_SHAPE, F32)],
        scratch_shapes=[units(TOTAL), units(MAIN_HALF + LATE_HALF), units(slot_units), pltpu.VMEM((4 * ROWS, W1), F32), pltpu.VMEM(ONE_SHAPES[1], BF16), pltpu.VMEM(ONE_SHAPES[0], F32), pltpu.VMEM(ONE_SHAPES[0], F32), dma((len(parts),)), dma((3 * count,)), dma((count,)), dma((count,)), dma(both), dma(both), dma(each), dma(each), pltpu.SemaphoreType.REGULAR((count, 5))],
        compiler_params=params(collective_id=0, has_side_effects=True),
        name="sum_grads",
    )(*parts, *squares, *acts)


def solution(mesh):
    data_devs = mesh.shape['data']

    def local_step(x_now, labels_now, x_next, up_one, down_one, merge_proj, up_two, down_two, head_proj, vel_up_one, vel_down_one, vel_merge_proj, vel_up_two, vel_down_two, vel_head_proj):
        images = x_now.shape[0]
        xn = x_now.reshape(4 * ROWS, W1)
        xf = x_next.reshape(4 * ROWS, W1)
        mid, merged, res0, ub1, vb1, mb, su1, sv1, sm = stage_one_now(xn, up_one, down_one, merge_proj)
        res1, ub2, vb2, su2, sv2, sh, dh, grad_pool = stage_two_now(res0, labels_now, up_two, down_two, head_proj.T, images * data_devs)
        du2, dv2, dm, grad_mid = stage_two_back(grad_pool, res0, res1, merged, ub2, vb2, mb)
        grads, scales = sum_grads((du2, dv2, dm, dh), (grad_mid, xn, mid, ub1, vb1), (su2, sv2, sm[None], sh[None], su1, sv1))
        res_f, nu1, nv1, nm, qu1, qv1, qm = stage_one_next(xf, scales, grads, (up_one, down_one, merge_proj), (vel_up_one, vel_down_one, vel_merge_proj))
        nu2, nv2, nh, qu2, qv2, qh, logits = stage_two_next(res_f, scales, grads, (up_two, down_two, head_proj.T), (vel_up_two, vel_down_two, vel_head_proj.T), images)
        return logits, nu1, nv1, nm, nu2, nv2, nh.T, qu1, qv1, qm, qu2, qv2, qh.T

    batch_split = P('data')
    in_specs = (batch_split,) * 3 + (P(),) * 12
    out_specs = (batch_split,) + (P(),) * 12
    return jax.shard_map(local_step, mesh=mesh, in_specs=in_specs, out_specs=out_specs, check_vma=False)
```

```python
import functools

import jax
import jax.numpy as jnp
from jax import lax
from jax.experimental import pallas as pl
from jax.experimental.pallas import tpu as pltpu
from jax.sharding import PartitionSpec as P

MOMENTUM = 0.9
TRUST = 0.1
LN_EPS = 1e-6
GELU_A = 2.0 * 0.7978845608028654
GELU_B = 4.0 * GELU_A * 0.044715
UNIT = 16
LANES = 128
UNIT_SIZE = UNIT * LANES
ROWS = 1568
ROWS_PAD = 1792
PER_IMAGE = 196
W1 = 128
W2 = 512
H1 = 512
H2 = 2048
CHUNK = 512
NCH = H2 // CHUNK
FCHUNK = 1024
NF = H2 // FCHUNK
TILE = 784
NT = ROWS // TILE
TOKENS = 4 * TILE
SPLITS = (784, 784)
HEAD_PAD = 1024
HEAD_ROWS = HEAD_PAD // (2 * NF)
HEAD_UNITS = HEAD_ROWS * W2 // UNIT_SIZE
HERE_AXES = (0, 1)
CHUNK_UNITS = CHUNK * W2 // UNIT_SIZE
F_UNITS = FCHUNK * W2 // UNIT_SIZE
SCALE_SHAPE = (UNIT, LANES)
ONE_SHAPES = [(2, W1, H1), (2, H1, W1), (W2, W2)]
UP_SHAPE, DOWN_SHAPE = (2, W2, H2), (2, H2, W2)
VMEM_LIMIT = 63 * 1024 * 1024
F32 = jnp.float32
BF16 = jnp.bfloat16


def dot_nn(lhs, rhs):
    return lax.dot_general(lhs, rhs, (((1,), (0,)), ((), ())), preferred_element_type=F32)


def dot_nt(lhs, rhs):
    return lax.dot_general(lhs, rhs, (((1,), (1,)), ((), ())), preferred_element_type=F32)


def dot_tn(lhs, rhs):
    return lax.dot_general(lhs, rhs, (((0,), (0,)), ((), ())), preferred_element_type=F32)


def row_mean(values):
    return jnp.mean(values, axis=-1, keepdims=True)


def row_sum(values):
    return jnp.sum(values, axis=-1, keepdims=True)


def scale_of(ref, index):
    return ref[pl.ds(index, 1), :1]


def ln_parts(values):
    centered = values - row_mean(values)
    variance = row_mean(centered * centered)
    inv = lax.rsqrt(variance + LN_EPS)
    return centered * inv, inv


def ln_back(normed, inv, grad):
    return inv * (grad - row_mean(grad) - normed * row_mean(grad * normed))


def normalize(values):
    return ln_parts(values)[0].astype(BF16)


def gelu_fwd(half):
    tan = jnp.tanh(half * (GELU_A + GELU_B * (half * half)))
    return half + half * tan


def gelu_both(half):
    sq = half * half
    tan = jnp.tanh(half * (GELU_A + GELU_B * sq))
    above = 1.0 + tan
    return half * above, above * (1.0 + (half * (1.0 - tan)) * (GELU_A + (3.0 * GELU_B) * sq))


def halve(weight):
    return (0.5 * weight).astype(BF16)


def fold_sq(mat):
    rows, cols = mat.shape
    return jnp.sum((mat * mat).reshape(rows // 8, 8, cols), axis=0)


def lars_block(weight, vel, grad, scale):
    new_vel = MOMENTUM * vel + scale * grad.astype(F32)
    return weight - new_vel, new_vel


def put_units(ref, start, mat):
    rows, cols = mat.shape
    groups = rows // UNIT
    for lane in range(cols // LANES):
        ref[pl.ds(start + lane * groups, groups)] = mat[:, lane * LANES:(lane + 1) * LANES].reshape(groups, UNIT, LANES)


def get_units(ref, start, rows, cols):
    groups = rows // UNIT
    parts = [ref[pl.ds(start + lane * groups, groups)].reshape(rows, LANES) for lane in range(cols // LANES)]
    return parts[0] if len(parts) == 1 else jnp.concatenate(parts, axis=1)


struct = jax.ShapeDtypeStruct


def unit_struct(count):
    return struct((count, UNIT, LANES), BF16)


def params(**kwargs):
    return pltpu.CompilerParams(vmem_limit_bytes=VMEM_LIMIT, **kwargs)


def whole(shape):
    zeros = (0,) * len(shape)
    return pl.BlockSpec(shape, lambda *_: zeros)


def token_parts(x_ref, x_s):
    x_s[...] = x_ref[...].astype(F32)
    return [x_s[pl.ds(quarter, TILE, stride=4), :] for quarter in range(4)]


def stage_one_tile(parts, ub, vb, mb):
    outs0, outs1 = [], []
    for resid in parts:
        for layer in range(2):
            normed = normalize(resid.astype(F32))
            act = gelu_fwd(dot_nn(normed, ub[layer])).astype(BF16)
            resid = (resid.astype(F32) + dot_nn(act, vb[layer])).astype(BF16)
            (outs0, outs1)[layer].append(resid)
    mid = jnp.concatenate(outs0, axis=1)
    merged = jnp.concatenate(outs1, axis=1)
    return mid, merged, dot_nn(merged, mb[...]).astype(BF16)


def rows_spec(rows, cols):
    return pl.BlockSpec((rows, cols), lambda i: (i, 0))


def stage_one_now(x, up_one, down_one, merge):
    def kernel(x_ref, u_ref, v_ref, m_ref, mid_ref, merged_ref, res_ref, ub_ref, vb_ref, mb_ref, su_ref, sv_ref, sm_ref, x_s):
        @pl.when(pl.program_id(0) == 0)
        def _():
            ub_ref[...] = halve(u_ref[...])
            vb_ref[...] = v_ref[...].astype(BF16)
            mb_ref[...] = m_ref[...].astype(BF16)
            for layer in range(2):
                su_ref[layer] = fold_sq(u_ref[layer])
                sv_ref[layer] = fold_sq(v_ref[layer])
            sm_ref[...] = fold_sq(m_ref[...])

        mid, merged, res = stage_one_tile(token_parts(x_ref, x_s), ub_ref, vb_ref, mb_ref)
        mid_ref[...] = mid
        merged_ref[...] = merged
        res_ref[...] = res

    tile = rows_spec(TILE, W2)
    act = struct((ROWS, W2), BF16)
    small = [(shape, BF16) for shape in ONE_SHAPES] + [((2, 8, H1), F32), ((2, 8, W1), F32), ((8, W2), F32)]
    return pl.pallas_call(
        kernel,
        grid=(NT,),
        in_specs=[rows_spec(TOKENS, W1)] + [whole(s) for s in ONE_SHAPES],
        out_specs=[tile] * 3 + [whole(s) for s, _ in small],
        out_shape=[act] * 3 + [struct(s, d) for s, d in small],
        scratch_shapes=[pltpu.VMEM((TOKENS, W1), F32)],
        compiler_params=params(),
        name="stage_one_now",
    )(x, up_one, down_one, merge)


def stage_one_next(x, scales, grads, weights, vels):
    def kernel(sc_ref, x_ref, u_ref, v_ref, m_ref, pu_ref, pv_ref, pm_ref, gu_ref, gv_ref, gm_ref, res_ref, nu_ref, nv_ref, nm_ref, qu_ref, qv_ref, qm_ref, ub_ref, vb_ref, mb_ref, x_s):
        @pl.when(pl.program_id(0) == 0)
        def _():
            for layer in range(2):
                nu_ref[layer], qu_ref[layer] = lars_block(u_ref[layer], pu_ref[layer], get_units(gu_ref, 32 * layer, W1, H1), scale_of(sc_ref, 6 + layer))
                nv_ref[layer], qv_ref[layer] = lars_block(v_ref[layer], pv_ref[layer], get_units(gv_ref, 32 * layer, H1, W1), scale_of(sc_ref, 8 + layer))
            nm_ref[...], qm_ref[...] = lars_block(m_ref[...], pm_ref[...], get_units(gm_ref, 0, W2, W2), scale_of(sc_ref, 4))
            ub_ref[...] = halve(nu_ref[...])
            vb_ref[...] = nv_ref[...].astype(BF16)
            mb_ref[...] = nm_ref[...].astype(BF16)

        res_ref[...] = stage_one_tile(token_parts(x_ref, x_s), ub_ref, vb_ref, mb_ref)[2]

    shapes = ONE_SHAPES
    units = [pl.BlockSpec((size, 16, 128), lambda i, at=at: (at, 0, 0)) for size, at in ((64, 38), (64, 39), (128, 16))]
    return pl.pallas_call(
        kernel,
        grid=(NT,),
        in_specs=[whole(SCALE_SHAPE), rows_spec(TOKENS, W1)] + [whole(s) for s in shapes] * 2 + units,
        out_specs=[rows_spec(TILE, W2)] + [whole(s) for s in shapes] * 2,
        out_shape=[struct((ROWS, W2), BF16)] + [struct(s, F32) for s in shapes] * 2,
        scratch_shapes=[pltpu.VMEM(s, BF16) for s in shapes] + [pltpu.VMEM((TOKENS, W1), F32)],
        compiler_params=params(),
        name="stage_one_next",
    )(scales, x, *weights, *vels, grads, grads, grads)


def row_parts():
    return [(sum(SPLITS[:index]), size) for index, size in enumerate(SPLITS)]


def stage_two_start(chunk, src_ref, dst_norm, acc_ref):
    for start, size in row_parts():
        resid = src_ref[start:start + size].astype(F32)
        dst_norm[start:start + size] = normalize(resid)
        acc_ref[start:start + size] = resid


def stage_two_step(norm_ref, acc_ref, ub, vb):
    for start, size in row_parts():
        act = gelu_fwd(dot_nn(norm_ref[start:start + size], ub)).astype(BF16)
        acc_ref[start:start + size] += dot_nn(act, vb)


def pool_images(resid_ref):
    cols = lax.broadcasted_iota(jnp.int32, (UNIT, ROWS_PAD), 1)
    base = lax.broadcasted_iota(jnp.int32, (UNIT, ROWS_PAD), 0) * PER_IMAGE
    mask = ((cols >= base) & (cols < base + PER_IMAGE) & (cols < ROWS)).astype(F32).astype(BF16)
    return dot_nn(mask, resid_ref[...]) * (1.0 / PER_IMAGE)


def head_block(layer, chunk, h_ref, classes):
    at = pl.multiple_of((layer * NF + chunk) * HEAD_ROWS, HEAD_ROWS)
    rows = at + lax.broadcasted_iota(jnp.int32, h_ref.shape, 0)
    return at, jnp.where(rows < classes, h_ref[...], 0.0)


def two_specs():
    u_spec = pl.BlockSpec((1, W2, FCHUNK), lambda l, j: (l, 0, j))
    v_spec = pl.BlockSpec((1, FCHUNK, W2), lambda l, j: (l, j, 0))
    return u_spec, v_spec, pl.BlockSpec((HEAD_ROWS, W2), lambda l, j: (l * NF + j, 0))


def by_layer(layer, chunk):
    return layer, 0, 0


def stage_two_now(res_in, labels, up_two, down_two, head, global_batch):
    classes = head.shape[0]
    images = labels.shape[0]

    def kernel(r_ref, lab_ref, u_ref, v_ref, h_ref, mid_ref, ub_ref, vb_ref, su_ref, sv_ref, sh_ref, dh_ref, gp_ref, norm_s, acc_s, res_s, hb_s):
        layer, chunk = pl.program_id(0), pl.program_id(1)

        @pl.when((layer == 0) & (chunk == 0))
        def _():
            sh_ref[...] = jnp.zeros_like(sh_ref)

        @pl.when(chunk == 0)
        def _():
            @pl.when(layer == 0)
            def _():
                stage_two_start(chunk, r_ref, norm_s, acc_s)

            @pl.when(layer == 1)
            def _():
                stage_two_start(chunk, mid_ref, norm_s, acc_s)
            su_ref[...] = jnp.zeros_like(su_ref)
            sv_ref[...] = jnp.zeros_like(sv_ref)

        ub = halve(u_ref[0])
        vb = v_ref[0].astype(BF16)
        ub_ref[0] = ub
        vb_ref[0] = halve(v_ref[0])
        su_ref[0] += fold_sq(u_ref[0])
        sv_ref[0] += fold_sq(v_ref[0])
        at, head_part = head_block(layer, chunk, h_ref, classes)
        sh_ref[...] += fold_sq(head_part)
        hb_s[pl.ds(at, HEAD_ROWS)] = head_part.astype(BF16)
        stage_two_step(norm_s, acc_s, ub, vb)

        @pl.when((chunk == NF - 1) & (layer == 0))
        def _():
            mid_ref[...] = acc_s[...].astype(BF16)

        @pl.when((chunk == NF - 1) & (layer == 1))
        def _():
            res_s[:ROWS] = acc_s[...].astype(BF16)
            res_s[ROWS:] = jnp.zeros((ROWS_PAD - ROWS, W2), BF16)
            normed, inv = ln_parts(pool_images(res_s))
            head_in = normed.astype(BF16)
            logits = dot_nt(head_in, hb_s[...])
            cols = lax.broadcasted_iota(jnp.int32, logits.shape, 1)
            rows = lax.broadcasted_iota(jnp.int32, logits.shape, 0)
            live = cols < classes
            top = jnp.max(jnp.where(live, logits, -jnp.inf), axis=-1, keepdims=True)
            expd = jnp.where(live, jnp.exp(logits - top), 0.0)
            probs = expd / row_sum(expd)
            target = jnp.zeros_like(cols)
            for image in range(images):
                target = jnp.where(rows == image, lab_ref[image], target)
            onehot = (cols == target).astype(F32)
            grad_logits = jnp.where(rows < images, (probs - onehot) / global_batch, 0.0).astype(BF16)
            grad_head = dot_tn(grad_logits, head_in).astype(BF16)
            for block in range(2 * NF):
                put_units(dh_ref, block * HEAD_UNITS, grad_head[block * HEAD_ROWS:(block + 1) * HEAD_ROWS])
            grad_pool = ln_back(normed, inv, dot_nn(grad_logits, hb_s[...])) / PER_IMAGE
            gp_ref[...] = jnp.zeros_like(gp_ref)
            gp_ref[:UNIT] = grad_pool.astype(BF16)

    u_spec, v_spec, h_spec = two_specs()
    return pl.pallas_call(
        kernel,
        grid=(2, NF),
        in_specs=[whole((ROWS, W2)), pl.BlockSpec(memory_space=pltpu.SMEM), u_spec, v_spec, h_spec],
        out_specs=[whole((ROWS, W2)), u_spec, v_spec, pl.BlockSpec((1, 8, FCHUNK), by_layer), pl.BlockSpec((1, 8, W2), by_layer), whole((8, W2)), whole((256, UNIT, LANES)), whole((LANES, W2))],
        out_shape=[struct((ROWS, W2), BF16), struct(UP_SHAPE, BF16), struct(DOWN_SHAPE, BF16), struct((2, 8, FCHUNK), F32), struct((2, 8, W2), F32), struct((8, W2), F32), unit_struct(256), struct((LANES, W2), BF16)],
        scratch_shapes=[pltpu.VMEM((ROWS, W2), BF16), pltpu.VMEM((ROWS, W2), F32), pltpu.VMEM((ROWS_PAD, W2), BF16), pltpu.VMEM((HEAD_PAD, W2), BF16)],
        compiler_params=params(),
        name="stage_two_now",
    )(res_in, labels, up_two, down_two, head)


def stage_two_next(res_in, scales, grads, weights, vels, images):
    classes = weights[2].shape[0]

    def kernel(sc_ref, r_ref, u_ref, v_ref, h_ref, pu_ref, pv_ref, ph_ref, gu_ref, gv_ref, gh_ref, nu_ref, nv_ref, nh_ref, qu_ref, qv_ref, qh_ref, out_ref, norm_s, acc_s, res_s, hb_s):
        layer, chunk = pl.program_id(0), pl.program_id(1)

        @pl.when(chunk == 0)
        def _():
            @pl.when(layer == 0)
            def _():
                stage_two_start(chunk, r_ref, norm_s, acc_s)

            @pl.when(layer == 1)
            def _():
                stage_two_start(chunk, res_s, norm_s, acc_s)

        new_u, qu_ref[0] = lars_block(u_ref[0], pu_ref[0], get_units(gu_ref, 0, W2, FCHUNK), scale_of(sc_ref, layer))
        nu_ref[0] = new_u
        for part in range(FCHUNK // CHUNK):
            rows = slice(part * CHUNK, (part + 1) * CHUNK)
            nv_ref[0, rows], qv_ref[0, rows] = lars_block(v_ref[0, rows], pv_ref[0, rows], get_units(gv_ref, part * CHUNK_UNITS, CHUNK, W2), scale_of(sc_ref, 2 + layer))
        nh_ref[...], qh_ref[...] = lars_block(h_ref[...], ph_ref[...], get_units(gh_ref, 0, HEAD_ROWS, W2), scale_of(sc_ref, 5))
        at, head_part = head_block(layer, chunk, nh_ref, classes)
        hb_s[pl.ds(at, HEAD_ROWS)] = head_part.astype(BF16)
        stage_two_step(norm_s, acc_s, halve(new_u), nv_ref[0].astype(BF16))

        @pl.when(chunk == NF - 1)
        def _():
            res_s[:ROWS] = acc_s[...].astype(BF16)

            @pl.when(layer == 1)
            def _():
                res_s[ROWS:] = jnp.zeros((ROWS_PAD - ROWS, W2), BF16)
                head_in = normalize(pool_images(res_s))
                out_ref[...] = dot_nt(head_in, hb_s[...])[:images, :classes]

    u_spec, v_spec, h_spec = two_specs()
    units = [pl.BlockSpec((size, UNIT, LANES), lambda l, j, base=base // size: (base + l * NF + j, 0, 0)) for size, base in ((F_UNITS, 0), (F_UNITS, 1024), (HEAD_UNITS, 2176))]
    return pl.pallas_call(
        kernel,
        grid=(2, NF),
        in_specs=[whole(SCALE_SHAPE), whole((ROWS, W2))] + [u_spec, v_spec, h_spec] * 2 + units,
        out_specs=[u_spec, v_spec, h_spec] * 2 + [whole((images, classes))],
        out_shape=[struct(UP_SHAPE, F32), struct(DOWN_SHAPE, F32), struct((classes, W2), F32)] * 2 + [struct((images, classes), F32)],
        scratch_shapes=[pltpu.VMEM((ROWS, W2), BF16), pltpu.VMEM((ROWS, W2), F32), pltpu.VMEM((ROWS_PAD, W2), BF16), pltpu.VMEM((HEAD_PAD, W2), BF16)],
        compiler_params=params(),
        name="stage_two_next",
    )(scales, res_in, *weights, *vels, grads, grads, grads)


def stage_two_back(grad_pool, res_in, res_mid, merged, up_b, down_b, merge_b):
    def kernel(gp_ref, r0_ref, r1_ref, m_ref, u_ref, v_ref, mw_ref, du_ref, dv_ref, dm_ref, gout_ref, g_s, gt_s, n_s, nt_s, act_s, pre_s, dn_s):
        step, chunk = pl.program_id(0), pl.program_id(1)

        @pl.when((step == 0) & (chunk == 0))
        def _():
            rows = lax.broadcasted_iota(jnp.int32, (ROWS, 128), 0)
            base = lax.broadcasted_iota(jnp.int32, (ROWS, 128), 1) * PER_IMAGE
            mask = ((rows >= base) & (rows < base + PER_IMAGE)).astype(F32).astype(BF16)
            g_s[...] = dot_nn(mask, gp_ref[...]).astype(BF16)
            gt_s[...] = jnp.zeros_like(gt_s)
            nt_s[...] = jnp.zeros_like(nt_s)
            gt_s[:, :ROWS] = g_s[...].T
            act_s[ROWS:] = jnp.zeros((ROWS_PAD - ROWS, CHUNK), BF16)
            pre_s[ROWS:] = jnp.zeros((ROWS_PAD - ROWS, CHUNK), BF16)

        def begin(src_ref):
            n_s[...] = normalize(src_ref[...].astype(F32))
            nt_s[:, :ROWS] = n_s[...].T
            dn_s[...] = jnp.zeros_like(dn_s)

        @pl.when((step == 0) & (chunk == 0))
        def _():
            begin(r1_ref)

        @pl.when((step == 1) & (chunk == 0))
        def _():
            begin(r0_ref)

        ub = u_ref[0]
        vb = v_ref[0]
        for start, size in row_parts():
            act, slope = gelu_both(dot_nn(n_s[start:start + size], ub))
            grad_pre = (dot_nt(g_s[start:start + size], vb) * slope).astype(BF16)
            act_s[start:start + size] = act.astype(BF16)
            pre_s[start:start + size] = grad_pre
            dn_s[start:start + size] += dot_nt(grad_pre, ub)
        put_units(du_ref, 0, dot_nn(nt_s[...], pre_s[...]).astype(BF16))
        put_units(dv_ref, 0, dot_nn(gt_s[...], act_s[...]).T.astype(BF16))

        def finish(src_ref):
            normed, inv = ln_parts(src_ref[...].astype(F32))
            g_s[...] = (ln_back(normed, inv + inv, dn_s[...]) + g_s[...].astype(F32)).astype(BF16)

        @pl.when((step == 0) & (chunk == NCH - 1))
        def _():
            finish(r1_ref)
            gt_s[:, :ROWS] = g_s[...].T

        @pl.when((step == 1) & (chunk == NCH - 1))
        def _():
            finish(r0_ref)
            gout_ref[...] = dot_nt(g_s[...], mw_ref[...]).astype(BF16)
            put_units(dm_ref, 0, dot_tn(m_ref[...], g_s[...]).astype(BF16))

    u_spec = pl.BlockSpec((1, W2, CHUNK), lambda l, j: (1 - l, 0, j))
    v_spec = pl.BlockSpec((1, CHUNK, W2), lambda l, j: (1 - l, j, 0))
    g_spec = pl.BlockSpec((CHUNK_UNITS, UNIT, LANES), lambda l, j: ((1 - l) * NCH + j, 0, 0))
    act = whole((ROWS, W2))
    return pl.pallas_call(
        kernel,
        grid=(2, NCH),
        in_specs=[whole((128, W2)), act, act, act, u_spec, v_spec, whole((W2, W2))],
        out_specs=[g_spec, g_spec, whole((128, UNIT, LANES)), act],
        out_shape=[unit_struct(1024), unit_struct(1024), unit_struct(128), struct((ROWS, W2), BF16)],
        scratch_shapes=[pltpu.VMEM((ROWS, W2), BF16), pltpu.VMEM((W2, ROWS_PAD), BF16), pltpu.VMEM((ROWS, W2), BF16), pltpu.VMEM((W2, ROWS_PAD), BF16), pltpu.VMEM((ROWS_PAD, CHUNK), BF16), pltpu.VMEM((ROWS_PAD, CHUNK), BF16), pltpu.VMEM((ROWS, W2), F32)],
        compiler_params=params(),
        name="stage_two_back",
    )(grad_pool, res_in, res_mid, merged, up_b, down_b, merge_b)


AXIS_STEP = (2, 8, 32)
MAIN_UNITS = (13, 13, 13, 13, 12, 12)
LATE_UNITS = (2, 2)
MAIN = tuple(range(len(MAIN_UNITS)))
LATE = tuple(range(len(MAIN_UNITS), len(MAIN_UNITS) + len(LATE_UNITS)))
MAIN_HALF = UNIT * sum(MAIN_UNITS)
LATE_HALF = UNIT * sum(LATE_UNITS)
TOTAL = 2 * (MAIN_HALF + LATE_HALF)
COUNTS = (512,) * 4 + (128, 256) + (32,) * 4
SEGMENTS = (1024, 1024, 128, 256)
LOOPS = ((0, 2), (2, 6), (6, 8))
HOPS = 6
PIECES = (0, 1)
BACKS = (0, 1, 2)


def stream_plan():
    plan, base, slot = [], 0, 0
    for index, units in enumerate(MAIN_UNITS + LATE_UNITS):
        hops = [((index // 2 + turn // 2) % 3, (index + turn) % 2) for turn in range(HOPS)]
        plan.append((units, base, slot, hops))
        base += UNIT * units
        slot += (UNIT + 1) * units
    return plan, slot


def sum_grads(parts, acts, squares):
    plan, slot_units = stream_plan()
    count = len(plan)

    def kernel(*refs):
        refs = list(refs)
        take = lambda number: [refs.pop(0) for _ in range(number)]
        part_refs, sq_refs = take(len(parts)), take(len(squares))
        g_ref, x_ref, mid_ref, u_ref, v_ref, out_ref, scale_ref = take(7)
        flat, pair_buf, slots, x_s, vh_s, du_s, dv_s, load_sem, out_sem, pair_send, pair_recv, back_send, back_recv, hop_send, hop_recv, ready = refs
        me = lax.axis_index('data')
        core = lax.rem(me, 2)
        peer = me + 1 - 2 * core
        partner, bit = {}, {}
        for axis, step in enumerate(AXIS_STEP):
            spot = lax.rem(me // step, 4)
            partner[axis, 0] = me + (1 - 2 * lax.rem(spot, 2)) * step
            partner[axis, 1] = me + (3 - 2 * spot) * step
            bit[axis, 0] = lax.rem((spot + 1) // 2, 2)
            bit[axis, 1] = spot // 2

        loads = [pltpu.make_async_copy(part_refs[k], flat.at[pl.ds(sum(SEGMENTS[:k]), size)], load_sem.at[k]) for k, size in enumerate(SEGMENTS)]
        for load in loads:
            load.start()
        barrier = pltpu.get_barrier_semaphore()
        for other in [peer] + list(partner.values()):
            pl.semaphore_signal(barrier, device_id=(other,), device_id_type=pl.DeviceIdType.MESH)
        x_s[...] = x_ref[...].astype(F32)
        vh_s[...] = halve(v_ref[...].astype(F32))
        du_s[...] = jnp.zeros_like(du_s)
        dv_s[...] = jnp.zeros_like(dv_s)
        pl.semaphore_wait(barrier, 1 + len(partner))
        for load in loads:
            load.wait()

        def send(src, dst, send_sem, recv_sem, device):
            copy = pltpu.make_async_remote_copy(src_ref=src, dst_ref=dst, send_sem=send_sem, recv_sem=recv_sem, device_id=(device,), device_id_type=pl.DeviceIdType.MESH)
            copy.start()
            return copy

        def add_in(start, src, src_start, units, blocks):
            def body(index, carry):
                at = pl.ds(start + index * units, units)
                flat[at] = flat[at] + src[pl.ds(src_start + index * units, units)]
                return carry
            lax.fori_loop(0, blocks, body, 0)

        def home(k, side):
            return plan[k][1] + (MAIN_HALF + side * LATE_HALF if k in LATE else side * MAIN_HALF)

        kept, gone = [[] for _ in plan], [[] for _ in plan]
        for k, (units, base, slot, hops) in enumerate(plan):
            start = home(k, core)
            for turn in range(4):
                size = (8 >> turn) * units
                flag = bit[hops[turn]]
                gone[k].append(start + (1 - flag) * size)
                start = start + flag * size
                kept[k].append(start)
        copies, pairs, backs, outs = {}, {}, {}, []

        def halves(k, start, turn):
            size = (4 >> turn) * plan[k][0]
            flag = bit[plan[k][3][turn + 1]]
            return [(start + (1 - flag) * size, size), (start + flag * size, size)]

        def pair_up(streams):
            for piece, side in enumerate((gone, kept)):
                for k in streams:
                    units, base = plan[k][:2]
                    at = side[k][0] - home(k, core)
                    pairs[k, piece] = send(flat.at[pl.ds(home(k, 1 - core) + at, 8 * units)], pair_buf.at[pl.ds(base + at, 8 * units)], pair_send.at[k, piece], pair_recv.at[k, piece], peer)

        def slot_at(k, turn):
            units, slot = plan[k][0], plan[k][2]
            return slot + sum((8 >> t) if t < 4 else 1 for t in range(turn)) * units

        def pieces_of(k, turn):
            return halves(k, gone[k][turn], turn) if turn < 3 else [(gone[k][3] if turn < 4 else kept[k][3], plan[k][0])]

        def hop(k, turn):
            for piece, (src, size) in enumerate(pieces_of(k, turn)):
                dst = slot_at(k, turn) + (src - gone[k][turn] if turn < 3 else 0)
                copies[k, turn, piece] = send(flat.at[pl.ds(src, size)], slots.at[pl.ds(dst, size)], hop_send.at[k, turn, piece], hop_recv.at[k, turn, piece], partner[plan[k][3][turn]])

        def first_hops(streams):
            for piece, side in enumerate((gone, kept)):
                for k in streams:
                    units, base = plan[k][:2]
                    pairs[k, piece].wait_recv()
                    add_in(side[k][0], pair_buf, base + side[k][0] - home(k, core), units, 8)
                    if piece == 0:
                        hop(k, 0)

        def tell(k, turn, device):
            pl.semaphore_signal(ready.at[k, turn], device_id=(device,), device_id_type=pl.DeviceIdType.MESH)

        def reduce_turn(streams, turn):
            if turn == HOPS - 1:
                for k in streams:
                    for piece in PIECES:
                        pairs[k, piece].wait_send()
                    tell(k, 4, peer)
                    for early in range(4):
                        for piece in range(len(pieces_of(k, early))):
                            copies[k, early, piece].wait_send()
                        tell(k, early, partner[plan[k][3][early]])
            if turn < 3:
                for piece, side in enumerate((gone, kept)):
                    for k in streams:
                        copies[k, turn, piece].wait_recv()
                        dst = side[k][turn + 1]
                        add_in(dst, slots, slot_at(k, turn) + dst - kept[k][turn], plan[k][0], 4 >> turn)
                        if piece == 0:
                            hop(k, turn + 1)
                return
            for k in streams:
                copies[k, turn, 0].wait_recv()
                if turn > 3:
                    copies[k, turn, 0].wait_send()
                add_in(kept[k][3], slots, slot_at(k, turn), plan[k][0], 1)
                if turn < HOPS - 1:
                    hop(k, turn + 1)
                else:
                    share(k, 3, 0)
                    share(k, 2, 0)

        def spread(k, turn):
            if turn > 2:
                return [(kept[k][3], plan[k][0])]
            return halves(k, kept[k][turn], turn)[::-1]

        def share(k, turn, piece):
            start, size = spread(k, turn)[piece]
            if piece == 0:
                pl.semaphore_wait(ready.at[k, turn], 1)
            at = 2 * HOPS - 3 - turn
            copies[k, at, piece] = send(flat.at[pl.ds(start, size)], flat.at[pl.ds(start, size)], hop_send.at[k, at, piece], hop_recv.at[k, at, piece], partner[plan[k][3][turn]])

        def put(region, index):
            copy = pltpu.make_async_copy(flat.at[region], out_ref.at[region], out_sem.at[index])
            copy.start()
            outs.append(copy)

        def back(k, index, start, size):
            region = pl.ds(start, size)
            backs[k, index] = send(flat.at[region], flat.at[region], back_send.at[k, index], back_recv.at[k, index], peer)
            put(region, 4 * k + index)

        def gather_turn(streams, turn):
            for piece in range(2 if turn < 3 else 1):
                for k in streams:
                    copies[k, 2 * HOPS - 3 - turn, piece].wait_recv()
                    if turn == 0:
                        back(k, 1 + piece, *halves(k, gone[k][0], 0)[1 - piece])
                    elif piece or turn > 2:
                        share(k, turn - 1, 1)
                        if turn > 1:
                            share(k, turn - 2, 0)
                        else:
                            pl.semaphore_wait(ready.at[k, 4], 1)
                            back(k, 0, kept[k][0], 8 * plan[k][0])

        def token_block(index, carry):
            quarter, tile = lax.rem(index, 4), index // 4
            rows = pl.ds(pl.multiple_of(tile * TILE, UNIT), TILE)
            cols = pl.ds(pl.multiple_of(quarter * W1, W1), W1)
            grad = g_ref[rows, cols]
            for layer in (1, 0):
                source = mid_ref[rows, cols].astype(F32) if layer else x_s[pl.ds(tile * TOKENS + quarter, TILE, stride=4), :]
                normed, inv = ln_parts(source)
                normed_b = normed.astype(BF16)
                act, slope = gelu_both(dot_nn(normed_b, u_ref[layer]))
                grad_pre = (dot_nt(grad, vh_s[layer]) * slope).astype(BF16)
                du_s[layer] += dot_tn(normed_b, grad_pre)
                dv_s[layer] += dot_tn(grad, act.astype(BF16))
                if layer:
                    grad = (ln_back(normed, inv + inv, dot_nt(grad_pre, u_ref[layer])) + grad.astype(F32)).astype(BF16)
            return carry

        pair_up(MAIN)
        for number, (low, high) in enumerate(LOOPS):
            lax.fori_loop(low, high, token_block, 0)
            if number == 0:
                first_hops(MAIN)
            elif number == 1:
                reduce_turn(MAIN, 0)
        for layer in range(2):
            late = sum(SEGMENTS) + layer * (LATE_HALF // 2)
            put_units(flat, late, du_s[layer].astype(BF16))
            put_units(flat, late + LATE_HALF, dv_s[layer].T.astype(BF16))
        pair_up(LATE)
        reduce_turn(MAIN, 1)
        first_hops(LATE)
        for turn in range(2, HOPS):
            reduce_turn(MAIN, turn)
            reduce_turn(LATE, turn - 2)
        gather_turn(MAIN, 3)
        reduce_turn(LATE, HOPS - 2)
        gather_turn(MAIN, 2)
        reduce_turn(LATE, HOPS - 1)
        gather_turn(MAIN, 1)
        for turn in (3, 2, 1, 0):
            gather_turn(LATE, turn)
        gather_turn(MAIN, 0)
        for k in range(count):
            for index in BACKS:
                backs[k, index].wait_recv()
            put(pl.ds(home(k, 1 - core), UNIT * plan[k][0]), 4 * k + 3)
        squares_list = [ref.at[row] for ref in sq_refs for row in range(ref.shape[0])]
        for index, size in enumerate(COUNTS):
            def body(step, total, first=sum(COUNTS[:index])):
                block = flat[pl.ds(first + step * UNIT, UNIT)].astype(F32)
                return total + jnp.sum(block * block, axis=HERE_AXES, keepdims=True)[0]
            grad_sq = row_sum(lax.fori_loop(0, size // UNIT, body, jnp.zeros((1, LANES), F32)))
            weight_sq = row_sum(jnp.sum(squares_list[index][...], axis=0, keepdims=True))
            scale_ref[pl.ds(index, 1), :] = jnp.broadcast_to(TRUST * (jnp.sqrt(weight_sq) / jnp.sqrt(grad_sq)), (1, LANES))
        for copy in outs:
            copy.wait()
        for k in range(count):
            for index in BACKS:
                backs[k, index].wait_send()
            for turn in range(4):
                for piece in range(len(spread(k, turn))):
                    copies[k, 2 * HOPS - 3 - turn, piece].wait_send()

    anywhere = pl.BlockSpec(memory_space=pl.ANY)
    vmem = pl.BlockSpec(memory_space=pltpu.VMEM)
    dma = pltpu.SemaphoreType.DMA
    units = lambda number: pltpu.VMEM((number, UNIT, LANES), BF16)
    both, each = (count, 3), (count, HOPS + 4, 2)
    return pl.pallas_call(
        kernel,
        in_specs=[anywhere] * len(parts) + [vmem] * (len(squares) + len(acts)),
        out_specs=[anywhere, vmem],
        out_shape=[unit_struct(TOTAL), struct(SCALE_SHAPE, F32)],
        scratch_shapes=[units(TOTAL), units(MAIN_HALF + LATE_HALF), units(slot_units), pltpu.VMEM((4 * ROWS, W1), F32), pltpu.VMEM(ONE_SHAPES[1], BF16), pltpu.VMEM(ONE_SHAPES[0], F32), pltpu.VMEM(ONE_SHAPES[0], F32), dma((len(parts),)), dma((4 * count,)), dma(both), dma(both), dma(both), dma(both), dma(each), dma(each), pltpu.SemaphoreType.REGULAR((count, 5))],
        compiler_params=params(collective_id=0, has_side_effects=True),
        name="sum_grads",
    )(*parts, *squares, *acts)


def solution(mesh):
    data_devs = mesh.shape['data']

    def local_step(x_now, labels_now, x_next, up_one, down_one, merge_proj, up_two, down_two, head_proj, vel_up_one, vel_down_one, vel_merge_proj, vel_up_two, vel_down_two, vel_head_proj):
        images = x_now.shape[0]
        xn = x_now.reshape(4 * ROWS, W1)
        xf = x_next.reshape(4 * ROWS, W1)
        mid, merged, res0, ub1, vb1, mb, su1, sv1, sm = stage_one_now(xn, up_one, down_one, merge_proj)
        res1, ub2, vb2, su2, sv2, sh, dh, grad_pool = stage_two_now(res0, labels_now, up_two, down_two, head_proj.T, images * data_devs)
        du2, dv2, dm, grad_mid = stage_two_back(grad_pool, res0, res1, merged, ub2, vb2, mb)
        grads, scales = sum_grads((du2, dv2, dm, dh), (grad_mid, xn, mid, ub1, vb1), (su2, sv2, sm[None], sh[None], su1, sv1))
        res_f, nu1, nv1, nm, qu1, qv1, qm = stage_one_next(xf, scales, grads, (up_one, down_one, merge_proj), (vel_up_one, vel_down_one, vel_merge_proj))
        nu2, nv2, nh, qu2, qv2, qh, logits = stage_two_next(res_f, scales, grads, (up_two, down_two, head_proj.T), (vel_up_two, vel_down_two, vel_head_proj.T), images)
        return logits, nu1, nv1, nm, nu2, nv2, nh.T, qu1, qv1, qm, qu2, qv2, qh.T

    batch_split = P('data')
    in_specs = (batch_split,) * 3 + (P(),) * 12
    out_specs = (batch_split,) + (P(),) * 12
    return jax.shard_map(local_step, mesh=mesh, in_specs=in_specs, out_specs=out_specs, check_vma=False)
```

```python
import functools

import jax
import jax.numpy as jnp
from jax import lax
from jax.experimental import pallas as pl
from jax.experimental.pallas import tpu as pltpu
from jax.sharding import PartitionSpec as P

MOMENTUM = 0.9
TRUST = 0.1
LN_EPS = 1e-6
GELU_A = 2.0 * 0.7978845608028654
GELU_B = 4.0 * GELU_A * 0.044715
UNIT = 16
LANES = 128
UNIT_SIZE = UNIT * LANES
ROWS = 1568
ROWS_PAD = 1792
PER_IMAGE = 196
W1 = 128
W2 = 512
H1 = 512
H2 = 2048
CHUNK = 512
NCH = H2 // CHUNK
FCHUNK = 1024
NF = H2 // FCHUNK
TILE = 784
NT = ROWS // TILE
TOKENS = 4 * TILE
SPLITS = (784, 784)
HEAD_PAD = 1024
HEAD_ROWS = HEAD_PAD // (2 * NF)
HEAD_UNITS = HEAD_ROWS * W2 // UNIT_SIZE
HERE_AXES = (0, 1)
CHUNK_UNITS = CHUNK * W2 // UNIT_SIZE
F_UNITS = FCHUNK * W2 // UNIT_SIZE
SCALE_SHAPE = (UNIT, LANES)
ONE_SHAPES = [(2, W1, H1), (2, H1, W1), (W2, W2)]
UP_SHAPE, DOWN_SHAPE = (2, W2, H2), (2, H2, W2)
VMEM_LIMIT = 63 * 1024 * 1024
F32 = jnp.float32
BF16 = jnp.bfloat16


def dot_nn(lhs, rhs):
    return lax.dot_general(lhs, rhs, (((1,), (0,)), ((), ())), preferred_element_type=F32)


def dot_nt(lhs, rhs):
    return lax.dot_general(lhs, rhs, (((1,), (1,)), ((), ())), preferred_element_type=F32)


def dot_tn(lhs, rhs):
    return lax.dot_general(lhs, rhs, (((0,), (0,)), ((), ())), preferred_element_type=F32)


def row_mean(values):
    return jnp.mean(values, axis=-1, keepdims=True)


def row_sum(values):
    return jnp.sum(values, axis=-1, keepdims=True)


def scale_of(ref, index):
    return ref[pl.ds(index, 1), :1]


def ln_parts(values):
    centered = values - row_mean(values)
    variance = row_mean(centered * centered)
    inv = lax.rsqrt(variance + LN_EPS)
    return centered * inv, inv


def ln_back(normed, inv, grad):
    return inv * (grad - row_mean(grad) - normed * row_mean(grad * normed))


def normalize(values):
    return ln_parts(values)[0].astype(BF16)


def gelu_fwd(half):
    tan = jnp.tanh(half * (GELU_A + GELU_B * (half * half)))
    return half + half * tan


def gelu_both(half):
    sq = half * half
    tan = jnp.tanh(half * (GELU_A + GELU_B * sq))
    above = 1.0 + tan
    return half * above, above * (1.0 + (half * (1.0 - tan)) * (GELU_A + (3.0 * GELU_B) * sq))


def halve(weight):
    return (0.5 * weight).astype(BF16)


def fold_sq(mat):
    rows, cols = mat.shape
    return jnp.sum((mat * mat).reshape(rows // 8, 8, cols), axis=0)


def lars_block(weight, vel, grad, scale):
    new_vel = MOMENTUM * vel + scale * grad.astype(F32)
    return weight - new_vel, new_vel


def put_units(ref, start, mat):
    rows, cols = mat.shape
    groups = rows // UNIT
    for lane in range(cols // LANES):
        ref[pl.ds(start + lane * groups, groups)] = mat[:, lane * LANES:(lane + 1) * LANES].reshape(groups, UNIT, LANES)


def get_units(ref, start, rows, cols):
    groups = rows // UNIT
    parts = [ref[pl.ds(start + lane * groups, groups)].reshape(rows, LANES) for lane in range(cols // LANES)]
    return parts[0] if len(parts) == 1 else jnp.concatenate(parts, axis=1)


struct = jax.ShapeDtypeStruct


def unit_struct(count):
    return struct((count, UNIT, LANES), BF16)


def params(**kwargs):
    return pltpu.CompilerParams(vmem_limit_bytes=VMEM_LIMIT, **kwargs)


def whole(shape):
    zeros = (0,) * len(shape)
    return pl.BlockSpec(shape, lambda *_: zeros)


def token_parts(x_ref, x_s):
    x_s[...] = x_ref[...].astype(F32)
    return [x_s[pl.ds(quarter, TILE, stride=4), :] for quarter in range(4)]


def stage_one_tile(parts, ub, vb, mb):
    outs0, outs1 = [], []
    for resid in parts:
        for layer in range(2):
            normed = normalize(resid.astype(F32))
            act = gelu_fwd(dot_nn(normed, ub[layer])).astype(BF16)
            resid = (resid.astype(F32) + dot_nn(act, vb[layer])).astype(BF16)
            (outs0, outs1)[layer].append(resid)
    mid = jnp.concatenate(outs0, axis=1)
    merged = jnp.concatenate(outs1, axis=1)
    return mid, merged, dot_nn(merged, mb[...]).astype(BF16)


def rows_spec(rows, cols):
    return pl.BlockSpec((rows, cols), lambda i: (i, 0))


def stage_one_now(x, up_one, down_one, merge):
    def kernel(x_ref, u_ref, v_ref, m_ref, mid_ref, merged_ref, res_ref, ub_ref, vb_ref, mb_ref, su_ref, sv_ref, sm_ref, x_s):
        @pl.when(pl.program_id(0) == 0)
        def _():
            ub_ref[...] = halve(u_ref[...])
            vb_ref[...] = v_ref[...].astype(BF16)
            mb_ref[...] = m_ref[...].astype(BF16)
            for layer in range(2):
                su_ref[layer] = fold_sq(u_ref[layer])
                sv_ref[layer] = fold_sq(v_ref[layer])
            sm_ref[...] = fold_sq(m_ref[...])

        mid, merged, res = stage_one_tile(token_parts(x_ref, x_s), ub_ref, vb_ref, mb_ref)
        mid_ref[...] = mid
        merged_ref[...] = merged
        res_ref[...] = res

    tile = rows_spec(TILE, W2)
    act = struct((ROWS, W2), BF16)
    small = [(shape, BF16) for shape in ONE_SHAPES] + [((2, 8, H1), F32), ((2, 8, W1), F32), ((8, W2), F32)]
    return pl.pallas_call(
        kernel,
        grid=(NT,),
        in_specs=[rows_spec(TOKENS, W1)] + [whole(s) for s in ONE_SHAPES],
        out_specs=[tile] * 3 + [whole(s) for s, _ in small],
        out_shape=[act] * 3 + [struct(s, d) for s, d in small],
        scratch_shapes=[pltpu.VMEM((TOKENS, W1), F32)],
        compiler_params=params(),
        name="stage_one_now",
    )(x, up_one, down_one, merge)


def stage_one_next(x, scales, grads, weights, vels):
    def kernel(sc_ref, x_ref, u_ref, v_ref, m_ref, pu_ref, pv_ref, pm_ref, gu_ref, gv_ref, gm_ref, res_ref, nu_ref, nv_ref, nm_ref, qu_ref, qv_ref, qm_ref, ub_ref, vb_ref, mb_ref, x_s):
        @pl.when(pl.program_id(0) == 0)
        def _():
            for layer in range(2):
                nu_ref[layer], qu_ref[layer] = lars_block(u_ref[layer], pu_ref[layer], get_units(gu_ref, 32 * layer, W1, H1), scale_of(sc_ref, 6 + layer))
                nv_ref[layer], qv_ref[layer] = lars_block(v_ref[layer], pv_ref[layer], get_units(gv_ref, 32 * layer, H1, W1), scale_of(sc_ref, 8 + layer))
            nm_ref[...], qm_ref[...] = lars_block(m_ref[...], pm_ref[...], get_units(gm_ref, 0, W2, W2), scale_of(sc_ref, 4))
            ub_ref[...] = halve(nu_ref[...])
            vb_ref[...] = nv_ref[...].astype(BF16)
            mb_ref[...] = nm_ref[...].astype(BF16)

        res_ref[...] = stage_one_tile(token_parts(x_ref, x_s), ub_ref, vb_ref, mb_ref)[2]

    shapes = ONE_SHAPES
    units = [pl.BlockSpec((size, 16, 128), lambda i, at=at: (at, 0, 0)) for size, at in ((64, 38), (64, 39), (128, 16))]
    return pl.pallas_call(
        kernel,
        grid=(NT,),
        in_specs=[whole(SCALE_SHAPE), rows_spec(TOKENS, W1)] + [whole(s) for s in shapes] * 2 + units,
        out_specs=[rows_spec(TILE, W2)] + [whole(s) for s in shapes] * 2,
        out_shape=[struct((ROWS, W2), BF16)] + [struct(s, F32) for s in shapes] * 2,
        scratch_shapes=[pltpu.VMEM(s, BF16) for s in shapes] + [pltpu.VMEM((TOKENS, W1), F32)],
        compiler_params=params(),
        name="stage_one_next",
    )(scales, x, *weights, *vels, grads, grads, grads)


def row_parts():
    return [(sum(SPLITS[:index]), size) for index, size in enumerate(SPLITS)]


def stage_two_start(chunk, src_ref, dst_norm, acc_ref):
    for start, size in row_parts():
        resid = src_ref[start:start + size].astype(F32)
        dst_norm[start:start + size] = normalize(resid)
        acc_ref[start:start + size] = resid


def stage_two_step(norm_ref, acc_ref, ub, vb):
    for start, size in row_parts():
        act = gelu_fwd(dot_nn(norm_ref[start:start + size], ub)).astype(BF16)
        acc_ref[start:start + size] += dot_nn(act, vb)


def pool_images(resid_ref):
    cols = lax.broadcasted_iota(jnp.int32, (UNIT, ROWS_PAD), 1)
    base = lax.broadcasted_iota(jnp.int32, (UNIT, ROWS_PAD), 0) * PER_IMAGE
    mask = ((cols >= base) & (cols < base + PER_IMAGE) & (cols < ROWS)).astype(F32).astype(BF16)
    return dot_nn(mask, resid_ref[...]) * (1.0 / PER_IMAGE)


def head_block(layer, chunk, h_ref, classes):
    at = pl.multiple_of((layer * NF + chunk) * HEAD_ROWS, HEAD_ROWS)
    rows = at + lax.broadcasted_iota(jnp.int32, h_ref.shape, 0)
    return at, jnp.where(rows < classes, h_ref[...], 0.0)


def two_specs():
    u_spec = pl.BlockSpec((1, W2, FCHUNK), lambda l, j: (l, 0, j))
    v_spec = pl.BlockSpec((1, FCHUNK, W2), lambda l, j: (l, j, 0))
    return u_spec, v_spec, pl.BlockSpec((HEAD_ROWS, W2), lambda l, j: (l * NF + j, 0))


def by_layer(layer, chunk):
    return layer, 0, 0


def stage_two_now(res_in, labels, up_two, down_two, head, global_batch):
    classes = head.shape[0]
    images = labels.shape[0]

    def kernel(r_ref, lab_ref, u_ref, v_ref, h_ref, mid_ref, ub_ref, vb_ref, su_ref, sv_ref, sh_ref, dh_ref, gp_ref, norm_s, acc_s, res_s, hb_s):
        layer, chunk = pl.program_id(0), pl.program_id(1)

        @pl.when((layer == 0) & (chunk == 0))
        def _():
            sh_ref[...] = jnp.zeros_like(sh_ref)

        @pl.when(chunk == 0)
        def _():
            @pl.when(layer == 0)
            def _():
                stage_two_start(chunk, r_ref, norm_s, acc_s)

            @pl.when(layer == 1)
            def _():
                stage_two_start(chunk, mid_ref, norm_s, acc_s)
            su_ref[...] = jnp.zeros_like(su_ref)
            sv_ref[...] = jnp.zeros_like(sv_ref)

        ub = halve(u_ref[0])
        vb = v_ref[0].astype(BF16)
        ub_ref[0] = ub
        vb_ref[0] = halve(v_ref[0])
        su_ref[0] += fold_sq(u_ref[0])
        sv_ref[0] += fold_sq(v_ref[0])
        at, head_part = head_block(layer, chunk, h_ref, classes)
        sh_ref[...] += fold_sq(head_part)
        hb_s[pl.ds(at, HEAD_ROWS)] = head_part.astype(BF16)
        stage_two_step(norm_s, acc_s, ub, vb)

        @pl.when((chunk == NF - 1) & (layer == 0))
        def _():
            mid_ref[...] = acc_s[...].astype(BF16)

        @pl.when((chunk == NF - 1) & (layer == 1))
        def _():
            res_s[:ROWS] = acc_s[...].astype(BF16)
            res_s[ROWS:] = jnp.zeros((ROWS_PAD - ROWS, W2), BF16)
            normed, inv = ln_parts(pool_images(res_s))
            head_in = normed.astype(BF16)
            logits = dot_nt(head_in, hb_s[...])
            cols = lax.broadcasted_iota(jnp.int32, logits.shape, 1)
            rows = lax.broadcasted_iota(jnp.int32, logits.shape, 0)
            live = cols < classes
            top = jnp.max(jnp.where(live, logits, -jnp.inf), axis=-1, keepdims=True)
            expd = jnp.where(live, jnp.exp(logits - top), 0.0)
            probs = expd / row_sum(expd)
            target = jnp.zeros_like(cols)
            for image in range(images):
                target = jnp.where(rows == image, lab_ref[image], target)
            onehot = (cols == target).astype(F32)
            grad_logits = jnp.where(rows < images, (probs - onehot) / global_batch, 0.0).astype(BF16)
            grad_head = dot_tn(grad_logits, head_in).astype(BF16)
            for block in range(2 * NF):
                put_units(dh_ref, block * HEAD_UNITS, grad_head[block * HEAD_ROWS:(block + 1) * HEAD_ROWS])
            grad_pool = ln_back(normed, inv, dot_nn(grad_logits, hb_s[...])) / PER_IMAGE
            gp_ref[...] = jnp.zeros_like(gp_ref)
            gp_ref[:UNIT] = grad_pool.astype(BF16)

    u_spec, v_spec, h_spec = two_specs()
    return pl.pallas_call(
        kernel,
        grid=(2, NF),
        in_specs=[whole((ROWS, W2)), pl.BlockSpec(memory_space=pltpu.SMEM), u_spec, v_spec, h_spec],
        out_specs=[whole((ROWS, W2)), u_spec, v_spec, pl.BlockSpec((1, 8, FCHUNK), by_layer), pl.BlockSpec((1, 8, W2), by_layer), whole((8, W2)), whole((256, UNIT, LANES)), whole((LANES, W2))],
        out_shape=[struct((ROWS, W2), BF16), struct(UP_SHAPE, BF16), struct(DOWN_SHAPE, BF16), struct((2, 8, FCHUNK), F32), struct((2, 8, W2), F32), struct((8, W2), F32), unit_struct(256), struct((LANES, W2), BF16)],
        scratch_shapes=[pltpu.VMEM((ROWS, W2), BF16), pltpu.VMEM((ROWS, W2), F32), pltpu.VMEM((ROWS_PAD, W2), BF16), pltpu.VMEM((HEAD_PAD, W2), BF16)],
        compiler_params=params(),
        name="stage_two_now",
    )(res_in, labels, up_two, down_two, head)


def stage_two_next(res_in, scales, grads, weights, vels, images):
    classes = weights[2].shape[0]

    def kernel(sc_ref, r_ref, u_ref, v_ref, h_ref, pu_ref, pv_ref, ph_ref, gu_ref, gv_ref, gh_ref, nu_ref, nv_ref, nh_ref, qu_ref, qv_ref, qh_ref, out_ref, norm_s, acc_s, res_s, hb_s):
        layer, chunk = pl.program_id(0), pl.program_id(1)

        @pl.when(chunk == 0)
        def _():
            @pl.when(layer == 0)
            def _():
                stage_two_start(chunk, r_ref, norm_s, acc_s)

            @pl.when(layer == 1)
            def _():
                stage_two_start(chunk, res_s, norm_s, acc_s)

        new_u, qu_ref[0] = lars_block(u_ref[0], pu_ref[0], get_units(gu_ref, 0, W2, FCHUNK), scale_of(sc_ref, layer))
        nu_ref[0] = new_u
        for part in range(FCHUNK // CHUNK):
            rows = slice(part * CHUNK, (part + 1) * CHUNK)
            nv_ref[0, rows], qv_ref[0, rows] = lars_block(v_ref[0, rows], pv_ref[0, rows], get_units(gv_ref, part * CHUNK_UNITS, CHUNK, W2), scale_of(sc_ref, 2 + layer))
        nh_ref[...], qh_ref[...] = lars_block(h_ref[...], ph_ref[...], get_units(gh_ref, 0, HEAD_ROWS, W2), scale_of(sc_ref, 5))
        at, head_part = head_block(layer, chunk, nh_ref, classes)
        hb_s[pl.ds(at, HEAD_ROWS)] = head_part.astype(BF16)
        stage_two_step(norm_s, acc_s, halve(new_u), nv_ref[0].astype(BF16))

        @pl.when(chunk == NF - 1)
        def _():
            res_s[:ROWS] = acc_s[...].astype(BF16)

            @pl.when(layer == 1)
            def _():
                res_s[ROWS:] = jnp.zeros((ROWS_PAD - ROWS, W2), BF16)
                head_in = normalize(pool_images(res_s))
                out_ref[...] = dot_nt(head_in, hb_s[...])[:images, :classes]

    u_spec, v_spec, h_spec = two_specs()
    units = [pl.BlockSpec((size, UNIT, LANES), lambda l, j, base=base // size: (base + l * NF + j, 0, 0)) for size, base in ((F_UNITS, 0), (F_UNITS, 1024), (HEAD_UNITS, 2176))]
    return pl.pallas_call(
        kernel,
        grid=(2, NF),
        in_specs=[whole(SCALE_SHAPE), whole((ROWS, W2))] + [u_spec, v_spec, h_spec] * 2 + units,
        out_specs=[u_spec, v_spec, h_spec] * 2 + [whole((images, classes))],
        out_shape=[struct(UP_SHAPE, F32), struct(DOWN_SHAPE, F32), struct((classes, W2), F32)] * 2 + [struct((images, classes), F32)],
        scratch_shapes=[pltpu.VMEM((ROWS, W2), BF16), pltpu.VMEM((ROWS, W2), F32), pltpu.VMEM((ROWS_PAD, W2), BF16), pltpu.VMEM((HEAD_PAD, W2), BF16)],
        compiler_params=params(),
        name="stage_two_next",
    )(scales, res_in, *weights, *vels, grads, grads, grads)


def stage_two_back(grad_pool, res_in, res_mid, merged, up_b, down_b, merge_b):
    def kernel(gp_ref, r0_ref, r1_ref, m_ref, u_ref, v_ref, mw_ref, du_ref, dv_ref, dm_ref, gout_ref, g_s, gt_s, n_s, nt_s, act_s, pre_s, dn_s):
        step, chunk = pl.program_id(0), pl.program_id(1)

        @pl.when((step == 0) & (chunk == 0))
        def _():
            rows = lax.broadcasted_iota(jnp.int32, (ROWS, 128), 0)
            base = lax.broadcasted_iota(jnp.int32, (ROWS, 128), 1) * PER_IMAGE
            mask = ((rows >= base) & (rows < base + PER_IMAGE)).astype(F32).astype(BF16)
            g_s[...] = dot_nn(mask, gp_ref[...]).astype(BF16)
            gt_s[...] = jnp.zeros_like(gt_s)
            nt_s[...] = jnp.zeros_like(nt_s)
            gt_s[:, :ROWS] = g_s[...].T
            act_s[ROWS:] = jnp.zeros((ROWS_PAD - ROWS, CHUNK), BF16)
            pre_s[ROWS:] = jnp.zeros((ROWS_PAD - ROWS, CHUNK), BF16)

        def begin(src_ref):
            n_s[...] = normalize(src_ref[...].astype(F32))
            nt_s[:, :ROWS] = n_s[...].T
            dn_s[...] = jnp.zeros_like(dn_s)

        @pl.when((step == 0) & (chunk == 0))
        def _():
            begin(r1_ref)

        @pl.when((step == 1) & (chunk == 0))
        def _():
            begin(r0_ref)

        ub = u_ref[0]
        vb = v_ref[0]
        for start, size in row_parts():
            act, slope = gelu_both(dot_nn(n_s[start:start + size], ub))
            grad_pre = (dot_nt(g_s[start:start + size], vb) * slope).astype(BF16)
            act_s[start:start + size] = act.astype(BF16)
            pre_s[start:start + size] = grad_pre
            dn_s[start:start + size] += dot_nt(grad_pre, ub)
        put_units(du_ref, 0, dot_nn(nt_s[...], pre_s[...]).astype(BF16))
        put_units(dv_ref, 0, dot_nn(gt_s[...], act_s[...]).T.astype(BF16))

        def finish(src_ref):
            normed, inv = ln_parts(src_ref[...].astype(F32))
            g_s[...] = (ln_back(normed, inv + inv, dn_s[...]) + g_s[...].astype(F32)).astype(BF16)

        @pl.when((step == 0) & (chunk == NCH - 1))
        def _():
            finish(r1_ref)
            gt_s[:, :ROWS] = g_s[...].T

        @pl.when((step == 1) & (chunk == NCH - 1))
        def _():
            finish(r0_ref)
            gout_ref[...] = dot_nt(g_s[...], mw_ref[...]).astype(BF16)
            put_units(dm_ref, 0, dot_tn(m_ref[...], g_s[...]).astype(BF16))

    u_spec = pl.BlockSpec((1, W2, CHUNK), lambda l, j: (1 - l, 0, j))
    v_spec = pl.BlockSpec((1, CHUNK, W2), lambda l, j: (1 - l, j, 0))
    g_spec = pl.BlockSpec((CHUNK_UNITS, UNIT, LANES), lambda l, j: ((1 - l) * NCH + j, 0, 0))
    act = whole((ROWS, W2))
    return pl.pallas_call(
        kernel,
        grid=(2, NCH),
        in_specs=[whole((128, W2)), act, act, act, u_spec, v_spec, whole((W2, W2))],
        out_specs=[g_spec, g_spec, whole((128, UNIT, LANES)), act],
        out_shape=[unit_struct(1024), unit_struct(1024), unit_struct(128), struct((ROWS, W2), BF16)],
        scratch_shapes=[pltpu.VMEM((ROWS, W2), BF16), pltpu.VMEM((W2, ROWS_PAD), BF16), pltpu.VMEM((ROWS, W2), BF16), pltpu.VMEM((W2, ROWS_PAD), BF16), pltpu.VMEM((ROWS_PAD, CHUNK), BF16), pltpu.VMEM((ROWS_PAD, CHUNK), BF16), pltpu.VMEM((ROWS, W2), F32)],
        compiler_params=params(),
        name="stage_two_back",
    )(grad_pool, res_in, res_mid, merged, up_b, down_b, merge_b)


AXIS_STEP = (2, 8, 32)
MAIN_UNITS = (13, 13, 13, 13, 12, 12)
LATE_UNITS = (2, 2)
MAIN = tuple(range(len(MAIN_UNITS)))
LATE = tuple(range(len(MAIN_UNITS), len(MAIN_UNITS) + len(LATE_UNITS)))
MAIN_HALF = UNIT * sum(MAIN_UNITS)
LATE_HALF = UNIT * sum(LATE_UNITS)
TOTAL = 2 * (MAIN_HALF + LATE_HALF)
COUNTS = (512,) * 4 + (128, 256) + (32,) * 4
SEGMENTS = (1024, 1024, 128, 256)
ENDS = (0, 1, 3, 5, 7, 8)
HOPS = 6
PIECES = (0, 1)
BACKS = (0, 1, 2)


def stream_plan():
    plan, base, slot = [], 0, 0
    for index, units in enumerate(MAIN_UNITS + LATE_UNITS):
        hops = [((index // 2 + turn // 2) % 3, (index + turn) % 2) for turn in range(HOPS)]
        plan.append((units, base, slot, hops))
        base += UNIT * units
        slot += (UNIT + 1) * units
    return plan, slot


def sum_grads(parts, acts, squares):
    plan, slot_units = stream_plan()
    count = len(plan)

    def kernel(*refs):
        refs = list(refs)
        take = lambda number: [refs.pop(0) for _ in range(number)]
        part_refs, sq_refs = take(len(parts)), take(len(squares))
        g_ref, x_ref, mid_ref, u_ref, v_ref, out_ref, scale_ref = take(7)
        flat, pair_buf, slots, x_s, vh_s, du_s, dv_s, load_sem, out_sem, pair_send, pair_recv, back_send, back_recv, hop_send, hop_recv, ready = refs
        me = lax.axis_index('data')
        core = lax.rem(me, 2)
        peer = me + 1 - 2 * core
        partner, bit = {}, {}
        for axis, step in enumerate(AXIS_STEP):
            spot = lax.rem(me // step, 4)
            partner[axis, 0] = me + (1 - 2 * lax.rem(spot, 2)) * step
            partner[axis, 1] = me + (3 - 2 * spot) * step
            bit[axis, 0] = lax.rem((spot + 1) // 2, 2)
            bit[axis, 1] = spot // 2

        loads = [pltpu.make_async_copy(part_refs[k], flat.at[pl.ds(sum(SEGMENTS[:k]), size)], load_sem.at[k]) for k, size in enumerate(SEGMENTS)]
        for load in loads:
            load.start()
        barrier = pltpu.get_barrier_semaphore()
        for other in [peer] + list(partner.values()):
            pl.semaphore_signal(barrier, device_id=(other,), device_id_type=pl.DeviceIdType.MESH)
        x_s[...] = x_ref[...].astype(F32)
        vh_s[...] = halve(v_ref[...].astype(F32))
        du_s[...] = jnp.zeros_like(du_s)
        dv_s[...] = jnp.zeros_like(dv_s)
        pl.semaphore_wait(barrier, 1 + len(partner))
        for load in loads:
            load.wait()

        def send(src, dst, send_sem, recv_sem, device):
            copy = pltpu.make_async_remote_copy(src_ref=src, dst_ref=dst, send_sem=send_sem, recv_sem=recv_sem, device_id=(device,), device_id_type=pl.DeviceIdType.MESH)
            copy.start()
            return copy

        def add_in(start, src, src_start, units, blocks):
            def body(index, carry):
                at = pl.ds(start + index * units, units)
                flat[at] = flat[at] + src[pl.ds(src_start + index * units, units)]
                return carry
            lax.fori_loop(0, blocks, body, 0)

        def home(k, side):
            return plan[k][1] + (MAIN_HALF + side * LATE_HALF if k in LATE else side * MAIN_HALF)

        kept, gone = [[] for _ in plan], [[] for _ in plan]
        for k, (units, base, slot, hops) in enumerate(plan):
            start = home(k, core)
            for turn in range(4):
                size = (8 >> turn) * units
                flag = bit[hops[turn]]
                gone[k].append(start + (1 - flag) * size)
                start = start + flag * size
                kept[k].append(start)
        copies, pairs, backs, outs = {}, {}, {}, []

        def halves(k, start, turn):
            size = (4 >> turn) * plan[k][0]
            flag = bit[plan[k][3][turn + 1]]
            return [(start + (1 - flag) * size, size), (start + flag * size, size)]

        def pair_up(streams):
            for piece, side in enumerate((gone, kept)):
                for k in streams:
                    units, base = plan[k][:2]
                    at = side[k][0] - home(k, core)
                    pairs[k, piece] = send(flat.at[pl.ds(home(k, 1 - core) + at, 8 * units)], pair_buf.at[pl.ds(base + at, 8 * units)], pair_send.at[k, piece], pair_recv.at[k, piece], peer)

        def slot_at(k, turn):
            units, slot = plan[k][0], plan[k][2]
            return slot + sum((8 >> t) if t < 4 else 1 for t in range(turn)) * units

        def pieces_of(k, turn):
            return halves(k, gone[k][turn], turn) if turn < 3 else [(gone[k][3] if turn < 4 else kept[k][3], plan[k][0])]

        def hop(k, turn):
            for piece, (src, size) in enumerate(pieces_of(k, turn)):
                dst = slot_at(k, turn) + (src - gone[k][turn] if turn < 3 else 0)
                copies[k, turn, piece] = send(flat.at[pl.ds(src, size)], slots.at[pl.ds(dst, size)], hop_send.at[k, turn, piece], hop_recv.at[k, turn, piece], partner[plan[k][3][turn]])

        def first_hops(streams):
            for piece, side in enumerate((gone, kept)):
                for k in streams:
                    units, base = plan[k][:2]
                    pairs[k, piece].wait_recv()
                    add_in(side[k][0], pair_buf, base + side[k][0] - home(k, core), units, 8)
                    if piece == 0:
                        hop(k, 0)

        def tell(k, turn, device):
            pl.semaphore_signal(ready.at[k, turn], device_id=(device,), device_id_type=pl.DeviceIdType.MESH)

        def reduce_turn(streams, turn, pieces=PIECES):
            if turn == HOPS - 1:
                for k in streams:
                    for piece in PIECES:
                        pairs[k, piece].wait_send()
                    tell(k, 4, peer)
                    for early in range(4):
                        for piece in range(len(pieces_of(k, early))):
                            copies[k, early, piece].wait_send()
                        tell(k, early, partner[plan[k][3][early]])
            if turn < 3:
                for piece in pieces:
                    for k in streams:
                        copies[k, turn, piece].wait_recv()
                        dst = (gone, kept)[piece][k][turn + 1]
                        add_in(dst, slots, slot_at(k, turn) + dst - kept[k][turn], plan[k][0], 4 >> turn)
                        if piece == 0:
                            hop(k, turn + 1)
                return
            for k in streams:
                copies[k, turn, 0].wait_recv()
                if turn > 3:
                    copies[k, turn, 0].wait_send()
                add_in(kept[k][3], slots, slot_at(k, turn), plan[k][0], 1)
                if turn < HOPS - 1:
                    hop(k, turn + 1)
                else:
                    share(k, 3, 0)
                    share(k, 2, 0)

        def spread(k, turn):
            if turn > 2:
                return [(kept[k][3], plan[k][0])]
            return halves(k, kept[k][turn], turn)[::-1]

        def share(k, turn, piece):
            start, size = spread(k, turn)[piece]
            if piece == 0:
                pl.semaphore_wait(ready.at[k, turn], 1)
            at = 2 * HOPS - 3 - turn
            copies[k, at, piece] = send(flat.at[pl.ds(start, size)], flat.at[pl.ds(start, size)], hop_send.at[k, at, piece], hop_recv.at[k, at, piece], partner[plan[k][3][turn]])

        def put(region, index):
            copy = pltpu.make_async_copy(flat.at[region], out_ref.at[region], out_sem.at[index])
            copy.start()
            outs.append(copy)

        def back(k, index, start, size):
            region = pl.ds(start, size)
            backs[k, index] = send(flat.at[region], flat.at[region], back_send.at[k, index], back_recv.at[k, index], peer)
            put(region, 4 * k + index)

        def gather_turn(streams, turn):
            for piece in range(2 if turn < 3 else 1):
                for k in streams:
                    copies[k, 2 * HOPS - 3 - turn, piece].wait_recv()
                    if turn == 0:
                        back(k, 1 + piece, *halves(k, gone[k][0], 0)[1 - piece])
                    elif piece or turn > 2:
                        share(k, turn - 1, 1)
                        if turn > 1:
                            share(k, turn - 2, 0)
                        else:
                            pl.semaphore_wait(ready.at[k, 4], 1)
                            back(k, 0, kept[k][0], 8 * plan[k][0])

        def token_block(index, carry):
            quarter, tile = lax.rem(index, 4), index // 4
            rows = pl.ds(pl.multiple_of(tile * TILE, UNIT), TILE)
            cols = pl.ds(pl.multiple_of(quarter * W1, W1), W1)
            grad = g_ref[rows, cols]
            for layer in (1, 0):
                source = mid_ref[rows, cols].astype(F32) if layer else x_s[pl.ds(tile * TOKENS + quarter, TILE, stride=4), :]
                normed, inv = ln_parts(source)
                normed_b = normed.astype(BF16)
                act, slope = gelu_both(dot_nn(normed_b, u_ref[layer]))
                grad_pre = (dot_nt(grad, vh_s[layer]) * slope).astype(BF16)
                du_s[layer] += dot_tn(normed_b, grad_pre)
                dv_s[layer] += dot_tn(grad, act.astype(BF16))
                if layer:
                    grad = (ln_back(normed, inv + inv, dot_nt(grad_pre, u_ref[layer])) + grad.astype(F32)).astype(BF16)
            return carry

        def after_blocks(number):
            if number < 1:
                first_hops(MAIN)
            elif number < 2:
                reduce_turn(MAIN, 0, PIECES[:1])
            elif number < 3:
                reduce_turn(MAIN, 0, PIECES[1:])
                reduce_turn(MAIN, 1)
            else:
                reduce_turn(MAIN, number - 1)

        pair_up(MAIN)
        for number in range(len(ENDS) - 1):
            lax.fori_loop(ENDS[number], ENDS[number + 1], token_block, 0)
            after_blocks(number)
        for layer in range(2):
            late = sum(SEGMENTS) + layer * (LATE_HALF // 2)
            put_units(flat, late, du_s[layer].astype(BF16))
            put_units(flat, late + LATE_HALF, dv_s[layer].T.astype(BF16))
        pair_up(LATE)
        reduce_turn(MAIN, HOPS - 2)
        first_hops(LATE)
        reduce_turn(MAIN, HOPS - 1)
        reduce_turn(LATE, 0)
        for turn in (3, 2, 1):
            gather_turn(MAIN, turn)
            reduce_turn(LATE, 4 - turn)
        for turn in range(4, HOPS):
            reduce_turn(LATE, turn)
        for turn in reversed(range(4)):
            gather_turn(LATE, turn)
        gather_turn(MAIN, 0)
        for k in range(count):
            for index in BACKS:
                backs[k, index].wait_recv()
            put(pl.ds(home(k, 1 - core), UNIT * plan[k][0]), 4 * k + 3)
        squares_list = [ref.at[row] for ref in sq_refs for row in range(ref.shape[0])]
        for index, size in enumerate(COUNTS):
            def body(step, total, first=sum(COUNTS[:index])):
                block = flat[pl.ds(first + step * UNIT, UNIT)].astype(F32)
                return total + jnp.sum(block * block, axis=HERE_AXES, keepdims=True)[0]
            grad_sq = row_sum(lax.fori_loop(0, size // UNIT, body, jnp.zeros((1, LANES), F32)))
            weight_sq = row_sum(jnp.sum(squares_list[index][...], axis=0, keepdims=True))
            scale_ref[pl.ds(index, 1), :] = jnp.broadcast_to(TRUST * (jnp.sqrt(weight_sq) / jnp.sqrt(grad_sq)), (1, LANES))
        for copy in outs:
            copy.wait()
        for k in range(count):
            for index in BACKS:
                backs[k, index].wait_send()
            for turn in range(4):
                for piece in range(len(spread(k, turn))):
                    copies[k, 2 * HOPS - 3 - turn, piece].wait_send()

    anywhere = pl.BlockSpec(memory_space=pl.ANY)
    vmem = pl.BlockSpec(memory_space=pltpu.VMEM)
    dma = pltpu.SemaphoreType.DMA
    units = lambda number: pltpu.VMEM((number, UNIT, LANES), BF16)
    both, each = (count, 3), (count, HOPS + 4, 2)
    return pl.pallas_call(
        kernel,
        in_specs=[anywhere] * len(parts) + [vmem] * (len(squares) + len(acts)),
        out_specs=[anywhere, vmem],
        out_shape=[unit_struct(TOTAL), struct(SCALE_SHAPE, F32)],
        scratch_shapes=[units(TOTAL), units(MAIN_HALF + LATE_HALF), units(slot_units), pltpu.VMEM((4 * ROWS, W1), F32), pltpu.VMEM(ONE_SHAPES[1], BF16), pltpu.VMEM(ONE_SHAPES[0], F32), pltpu.VMEM(ONE_SHAPES[0], F32), dma((len(parts),)), dma((4 * count,)), dma(both), dma(both), dma(both), dma(both), dma(each), dma(each), pltpu.SemaphoreType.REGULAR((count, 5))],
        compiler_params=params(collective_id=0, has_side_effects=True),
        name="sum_grads",
    )(*parts, *squares, *acts)


def solution(mesh):
    data_devs = mesh.shape['data']

    def local_step(x_now, labels_now, x_next, up_one, down_one, merge_proj, up_two, down_two, head_proj, vel_up_one, vel_down_one, vel_merge_proj, vel_up_two, vel_down_two, vel_head_proj):
        images = x_now.shape[0]
        xn = x_now.reshape(4 * ROWS, W1)
        xf = x_next.reshape(4 * ROWS, W1)
        mid, merged, res0, ub1, vb1, mb, su1, sv1, sm = stage_one_now(xn, up_one, down_one, merge_proj)
        res1, ub2, vb2, su2, sv2, sh, dh, grad_pool = stage_two_now(res0, labels_now, up_two, down_two, head_proj.T, images * data_devs)
        du2, dv2, dm, grad_mid = stage_two_back(grad_pool, res0, res1, merged, ub2, vb2, mb)
        grads, scales = sum_grads((du2, dv2, dm, dh), (grad_mid, xn, mid, ub1, vb1), (su2, sv2, sm[None], sh[None], su1, sv1))
        res_f, nu1, nv1, nm, qu1, qv1, qm = stage_one_next(xf, scales, grads, (up_one, down_one, merge_proj), (vel_up_one, vel_down_one, vel_merge_proj))
        nu2, nv2, nh, qu2, qv2, qh, logits = stage_two_next(res_f, scales, grads, (up_two, down_two, head_proj.T), (vel_up_two, vel_down_two, vel_head_proj.T), images)
        return logits, nu1, nv1, nm, nu2, nv2, nh.T, qu1, qv1, qm, qu2, qv2, qh.T

    batch_split = P('data')
    in_specs = (batch_split,) * 3 + (P(),) * 12
    out_specs = (batch_split,) + (P(),) * 12
    return jax.shard_map(local_step, mesh=mesh, in_specs=in_specs, out_specs=out_specs, check_vma=False)
```
